256 devices in a mesh: row: 8 (over z_lo, x), col: 32 (over y, z_hi, core).
Axes of the slice: x: 4, y: 4, z: 8 (z_hi: 4, z_lo: 2; z = z_hi * 2 + z_lo), core: 2. Of those that a mesh axis runs over, the one named last changes fastest.
Arguments:
- matrix: bfloat16 [4096, 131072], P('row', 'col'), may hold values from -0.09375 to 0.09375
- measured: float32 [256, 4096], P(None, 'row'), may hold values from -160 to 160
- support: int32 [4, 2048], replicated, may hold values from 0 to 131071, as said below
Outputs:
- estimate: float32 [256, 131072], P('row', 'col')
- row_norms: float32 [131072], P('col')
- residual_energy: float32 [4], replicated
The draws below stay inside these ranges and needn't reach their ends.
Inputs may be any that keep to these rules, and one draw needn't show every extreme that they name: Each row of support lists 2048 distinct signal-row indices in increasing order; in every row, each aligned block of 4096 indices (the signal rows of one index of col) holds at most 128 of them, and some block exactly 128.
All inputs are finite; a program needn't handle non-finite values.
Results may differ from the reference program's by a relative error of at most 0.015.
Values may be sent and summed in bfloat16 or wider, within the bound.
A program may use at most 64 MiB of HBM per device.

```python
import math
import jax
import jax.numpy as jnp
from jax import lax

MB = 512
NB = 4096
L = 256
KB = 64
ITERS = 4
M = 4096
N = 131072
K = 2048
N_ROW = 8
N_COL = 32


def draw_measured(key, part):
    key_base, key_rows, key_signals = jax.random.split(key, 3)
    position = jnp.arange(M, dtype=jnp.float32) / max(M - 1, 1)
    rising = math.log(3.0)
    values = jax.random.normal(key_base, (L, M), jnp.float32)
    values = jnp.clip(values, -5.0, 5.0)
    row_scale = jnp.exp(rising * position + jax.random.uniform(key_rows, (M,), jnp.float32) * math.log(10.0 / 3.0)) / 3.0
    signal_scale = jnp.exp(jax.random.uniform(key_signals, (L,), jnp.float32) * math.log(10.0)) / math.sqrt(10.0)
    return values * row_scale[None, :] * signal_scale[:, None]


def draw_support(key, part):
    blocks = N // NB

    def one_iteration(iteration_key):
        key_order, key_shift, key_ranks = jax.random.split(iteration_key, 3)
        block_order = jax.random.permutation(key_order, blocks)
        shifts = jax.random.randint(key_shift, (blocks // 2,), 0, KB + 1).at[0].set(KB)
        counts = jnp.zeros((blocks,), jnp.int32).at[block_order[0::2]].set(KB + shifts).at[block_order[1::2]].set(KB - shifts)
        rank_table = jax.vmap(lambda block_key: jax.random.permutation(block_key, NB))(jax.random.split(key_ranks, blocks))
        chosen = (rank_table < counts[:, None]).reshape(-1)
        return jnp.nonzero(chosen, size=K)[0].astype(jnp.int32)
    return jax.vmap(one_iteration)(jax.random.split(key, ITERS))


def shard_levels(key, extent, cuts, least, largest):
    factor_of = 1.0
    for dim, shards_of in cuts:
        steps = jax.random.uniform(jax.random.fold_in(jax.random.fold_in(key, 6), dim), (shards_of,), jnp.float32, least / len(cuts), largest / len(cuts))
        factor_of = factor_of * jnp.repeat(jnp.exp(steps), extent[dim] // shards_of).reshape((-1,) + (1,) * (len(extent) - 1 - dim))
    return factor_of


def scatter_about(own_key, extent, deviation, bound, cuts=(), kind=jnp.bfloat16):
    result = deviation * jax.random.normal(own_key, extent, jnp.float32)
    if cuts:
        result = result * shard_levels(own_key, extent, cuts, -0.22, 0.18)
    return jnp.clip(result, -bound, bound).astype(kind)


def setup_inputs(seed: int = 0) -> dict:
    key_of = jax.random.split(jax.random.key(seed), 4)
    return {
        "matrix": scatter_about(key_of[0], (M, N), M ** -0.5, 0.09375, ((0, 8), (1, 32))),
        "measured": draw_measured(jax.random.fold_in(key_of[3], 71), 0),
        "support": draw_support(jax.random.fold_in(key_of[3], 71), 0),
    }


STEP_SIZE = 0.25

def predict(matrix, current_half):

    def add_block(block, summed):
        start_col = (block * NB).astype(jnp.int32)
        columns = lax.dynamic_slice_in_dim(matrix, start_col, NB, 1)
        signal_cols = lax.dynamic_slice_in_dim(current_half, start_col, NB, 1)
        return summed + lax.dot_general(signal_cols, columns, (((1,), (1,)), ((), ())), preferred_element_type=jnp.float32)
    return lax.fori_loop(0, N_COL, add_block, jnp.zeros((L, MB * N_ROW), jnp.float32))

def descend(matrix, residual_half):

    def one_block(block):
        start_col = (block * NB).astype(jnp.int32)
        columns = lax.dynamic_slice_in_dim(matrix, start_col, NB, 1)
        summed = jnp.zeros((L, NB), jnp.float32)
        for group_index in range(N_ROW):
            part_sum = jnp.dot(residual_half[:, group_index * MB:(group_index + 1) * MB], columns[group_index * MB:(group_index + 1) * MB], preferred_element_type=jnp.float32)
            rounded = lax.optimization_barrier(part_sum.astype(jnp.bfloat16))
            summed = summed + rounded.astype(jnp.float32)
        return summed
    blocks_out = lax.map(one_block, jnp.arange(N_COL, dtype=jnp.int32))
    return jnp.transpose(blocks_out, (1, 0, 2)).reshape(L, N_COL * NB)

def reference(matrix, measured, support):
    total_cols = NB * N_COL
    current = jnp.zeros((L, total_cols), jnp.float32)
    energies = []
    stepped = current
    for iteration in range(ITERS):
        if iteration == 0:
            residual = measured
        else:
            residual = measured - predict(matrix, current.astype(jnp.bfloat16))
        energies.append(jnp.sum(residual * residual) / (L * MB * N_ROW))
        gradient = descend(matrix, residual.astype(jnp.bfloat16))
        stepped = current + STEP_SIZE * gradient
        keep_mask = jnp.zeros((total_cols,), jnp.float32).at[support[iteration]].set(1.0)
        current = stepped * keep_mask[None, :]
    row_norms = jnp.sqrt(lax.optimization_barrier(jnp.sum(stepped * stepped, axis=0)))
    return (current, row_norms, jnp.stack(energies))
```

```python
import functools

import jax
import jax.numpy as jnp
from jax import lax
from jax.experimental import pallas as pl
from jax.experimental.pallas import tpu as pltpu
from jax.sharding import PartitionSpec as P

KMAX = 128
STEP_SIZE = 0.25
CORES = 2
NEAR = (((1,), (1,)), ((), ()))
F32 = jnp.float32
BF16 = jnp.bfloat16


def iota(shape, dim):
    return lax.broadcasted_iota(jnp.int32, shape, dim)


def window(line, start, width):
    count = line.shape[1]
    below = jnp.sum(jnp.where(line < start, 1.0, 0.0), axis=1, keepdims=True)
    upto = jnp.sum(jnp.where(line < start + width, 1.0, 0.0), axis=1, keepdims=True)
    place = iota((KMAX, count), 1) - iota((KMAX, count), 0)
    local = (line - start).astype(F32)
    found = jnp.sum(
        jnp.where(place == below.astype(jnp.int32), local, 0.0), axis=1, keepdims=True
    )
    there = iota((KMAX, 1), 0).astype(F32) < upto - below
    return jnp.where(there, found, -1.0).astype(jnp.int32)


def one_hot(index, first, width):
    return jnp.where(iota((KMAX, width), 1) + first == index, 1.0, 0.0)


def split3(value):
    high = value.astype(BF16)
    rest = value - high.astype(F32)
    middle = rest.astype(BF16)
    low = (rest - middle.astype(F32)).astype(BF16)
    return jnp.concatenate([high, middle, low], axis=0)


def add3(value):
    third = value.shape[0] // 3
    return value[:third] + value[third : 2 * third] + value[2 * third :]


def kernel(
    shape,
    support,
    measured,
    matrix,
    estimate,
    norms,
    energies,
    a_block,
    index_own,
    index_held,
    image,
    kept,
    first_send,
    first_recv,
    slope_send,
    slope_recv,
    current_all,
    held,
    seen_all,
    moved_send,
    moved_recv,
    residual_all,
    grad_send,
    grad_recv,
    norm_all,
    load_sem,
    send_sem,
    recv_sem,
    grad_ssem,
    grad_rsem,
):
    rows, far, high, total_count = shape
    width = matrix.shape[1]
    depth = matrix.shape[0]
    group = measured.shape[0] // rows
    steps = support.shape[0]
    chunk = grad_send.shape[3]
    chunks = width // chunk
    i = lax.axis_index("row")
    col = lax.axis_index("col")
    core = lax.rem(col, CORES)
    h = lax.rem(col // CORES, high)
    y = col // (CORES * high)
    q = y * CORES + core

    def at(yy, hh, cc):
        return (yy * high + hh) * CORES + cc

    def member(k):
        return at(k // CORES, h, lax.rem(k, CORES))

    sems = iter(range(1000))
    pending = []

    def remote(src, dst, where, slot):
        return pltpu.make_async_remote_copy(
            src_ref=src,
            dst_ref=dst,
            send_sem=send_sem.at[slot],
            recv_sem=recv_sem.at[slot],
            device_id=where,
            device_id_type=pl.DeviceIdType.MESH,
        )

    row_peers = [(lax.rem(i + d, rows), col) for d in range(1, rows)]
    y_peers = [(i, at(lax.rem(y + d, far), h, core)) for d in range(1, far)]
    y_from = [lax.rem(y - d + far, far) for d in range(1, far)]
    h_peers = [(i, at(y, lax.rem(h + d, high), core)) for d in range(1, high)]
    h_from = [lax.rem(h - d + high, high) for d in range(1, high)]
    partner = (i, at(y, h, 1 - core))

    barrier = pltpu.get_barrier_semaphore()
    for peer in row_peers + y_peers + h_peers + [partner]:
        pl.semaphore_signal(
            barrier, inc=1, device_id=peer, device_id_type=pl.DeviceIdType.MESH
        )
    on_diagonal = i == q
    for k in range(rows):

        @pl.when(jnp.logical_not(jnp.logical_and(on_diagonal, i == k)))
        def _():
            pl.semaphore_signal(
                barrier,
                inc=1,
                device_id=(k, member(i)),
                device_id_type=pl.DeviceIdType.MESH,
            )

    loads = [
        pltpu.make_async_copy(
            matrix.at[:, pl.ds(c * chunk, chunk)],
            a_block.at[:, pl.ds(c * chunk, chunk)],
            load_sem.at[c],
        )
        for c in range(chunks)
    ]
    for load in loads:
        load.start()

    for t in range(steps):
        index_own[t] = window(support[t : t + 1, :], col * width, width)

    image[...] = jnp.zeros_like(image)
    for c in range(chunks):
        loads[c].wait()
        hot = jnp.concatenate(
            [one_hot(index_own[t], c * chunk, chunk).astype(BF16) for t in range(steps - 1)],
            axis=0,
        )
        image[...] += lax.dot_general(
            hot, a_block[:, c * chunk : (c + 1) * chunk], NEAR, preferred_element_type=F32
        )
    for t in range(steps - 1):
        kept[t, q] = image[t * KMAX : (t + 1) * KMAX, :].astype(BF16)

    first = lax.dot_general(
        measured[...].astype(BF16), kept[0, q], NEAR, preferred_element_type=F32
    ).astype(BF16)
    for k in range(rows):
        first_send[k] = first[k * group : (k + 1) * group, :]

    pl.semaphore_wait(barrier, len(row_peers + y_peers + h_peers) + 1 + rows - jnp.where(on_diagonal, 1, 0))

    base = [next(sems) for _ in range(rows)]
    first_copies = []
    for k in range(rows):
        copy = pltpu.make_async_remote_copy(
            src_ref=first_send.at[k],
            dst_ref=first_recv.at[i],
            send_sem=send_sem.at[base[k]],
            recv_sem=recv_sem.at[i],
            device_id=(q, member(k)),
            device_id_type=pl.DeviceIdType.MESH,
        )
        other = jnp.logical_not(jnp.logical_and(on_diagonal, q == k))
        pl.when(other)(copy.start)

        @pl.when(jnp.logical_not(other))
        def _():
            first_recv[i] = first_send[k]

        first_copies.append((other, copy))

    spread = []
    for t in range(steps - 1):
        to_y = [
            remote(kept.at[t, q], kept.at[t, q], peer, next(sems)) for peer in y_peers
        ]
        to_partner = remote(kept.at[t, q], kept.at[t, q], partner, next(sems))
        relay_slots = [next(sems) for _ in y_peers]
        for copy in to_y:
            copy.start()
        to_partner.start()
        pending += to_y + [to_partner]
        spread.append((to_y, to_partner, relay_slots))

    def gather(t, buffer, parts):
        to_y, to_partner, relay_slots = parts
        relays = []
        for n, copy in enumerate(to_y):
            copy.wait_recv()
            slot = y_from[n] * CORES + core
            relay = remote(buffer.at[slot], buffer.at[slot], partner, relay_slots[n])
            relay.start()
            relays.append(relay)
        to_partner.wait_recv()
        for relay in relays:
            relay.wait_recv()
        pending.extend(relays)

    for t in range(steps - 1):
        index_held[t] = window(support[t : t + 1, :], member(i) * width, width)

    def carried(t, value):
        diagonal = iota((KMAX, KMAX), 0) == iota((KMAX, KMAX), 1)
        after = jnp.sum(
            jnp.where(diagonal, index_held[t + 1].astype(F32), 0.0), axis=0, keepdims=True
        ).astype(jnp.int32)
        before = index_held[t]
        same = jnp.where(jnp.logical_and(before == after, before >= 0), 1.0, 0.0).astype(BF16)
        return add3(jnp.dot(split3(value), same, preferred_element_type=F32))

    for k in range(rows):
        self_here = jnp.logical_and(on_diagonal, i == k)
        arrived = pltpu.make_async_remote_copy(
            src_ref=first_send.at[k],
            dst_ref=first_recv.at[k],
            send_sem=send_sem.at[base[k]],
            recv_sem=recv_sem.at[k],
            device_id=(q, member(k)),
            device_id_type=pl.DeviceIdType.MESH,
        )
        pl.when(jnp.logical_not(self_here))(arrived.wait_recv)
    current = STEP_SIZE * jnp.sum(first_recv[...].astype(F32), axis=0)

    own_measured = measured[pl.ds(pl.multiple_of(q * group, group), group), :]
    energy = [jnp.sum(own_measured * own_measured)]
    for t in range(steps - 1):
        if t > 0:
            gather(t, kept.at[t], spread[t])
            slope = lax.dot_general(
                residual.astype(BF16),
                kept[t].reshape(rows * KMAX, depth),
                NEAR,
                preferred_element_type=F32,
            ).astype(BF16)
            for k in range(rows):
                slope_send[t - 1, k] = slope[:, k * KMAX : (k + 1) * KMAX]
            copies = []
            for d, peer in enumerate(row_peers):
                copies.append(
                    remote(
                        slope_send.at[t - 1, peer[0]], slope_recv.at[t - 1, d], peer, next(sems)
                    )
                )
                copies[-1].start()
            carry = carried(t - 1, held[...])
            for copy in copies:
                copy.wait_recv()
            pending += copies
            gathered = slope_send[t - 1, i].astype(F32) + jnp.sum(
                slope_recv[t - 1].astype(F32), axis=0
            )
            current = carry + STEP_SIZE * gathered
        held[...] = current
        current_all[t, i] = current.astype(BF16)
        copies = [
            remote(current_all.at[t, i], current_all.at[t, i], peer, next(sems))
            for peer in row_peers
        ]
        for copy in copies:
            copy.start()
        pending += copies
        if t == steps - 2:
            moved_send[...] = current
            move = remote(moved_send, moved_recv, (q, member(i)), next(sems))
            pl.when(jnp.logical_not(on_diagonal))(move.start)

            @pl.when(on_diagonal)
            def _():
                moved_recv[...] = moved_send[...]

        if t == 0:
            gather(t, kept.at[t], spread[t])
        for copy in copies:
            copy.wait_recv()
        signals = jnp.concatenate([current_all[t, k] for k in range(rows)], axis=1)
        seen_all[t, h] = jnp.dot(
            signals, kept[t].reshape(rows * KMAX, depth), preferred_element_type=F32
        ).astype(BF16)
        copies = [
            remote(seen_all.at[t, h], seen_all.at[t, h], peer, next(sems)) for peer in h_peers
        ]
        for copy in copies:
            copy.start()
        for copy in copies:
            copy.wait_recv()
        pending += copies
        residual = own_measured - jnp.sum(seen_all[t].astype(F32), axis=0)
        energy.append(jnp.sum(residual * residual))

    lanes = iota((16, depth), 1)
    values = jnp.zeros((16, depth), F32)
    for t in range(steps):
        values = jnp.where(lanes == t, energy[t], values)
    top = values.astype(BF16).astype(F32)
    mid = (values - top).astype(BF16).astype(F32)
    low = values - top - mid
    line = iota((16, depth), 0)
    values = jnp.where(line == 0, top, jnp.where(line == 1, mid, jnp.where(line == 2, low, 0.0)))
    residual_all[q] = jnp.concatenate([residual.astype(BF16), values.astype(BF16)], axis=0)
    to_y = [remote(residual_all.at[q], residual_all.at[q], peer, next(sems)) for peer in y_peers]
    to_partner = remote(residual_all.at[q], residual_all.at[q], partner, next(sems))
    for copy in to_y:
        copy.start()
    to_partner.start()
    pending += to_y + [to_partner]
    gather(0, residual_all, (to_y, to_partner, [next(sems) for _ in y_peers]))

    energy_rows = jnp.sum(
        jnp.sum(residual_all[:, group:, :KMAX].astype(F32), axis=0), axis=0, keepdims=True
    )
    norm_all[i, :, width:] = energy_rows

    all_signals = jnp.concatenate([residual_all[k, :group, :] for k in range(rows)], axis=0)

    def grad_copy(c, d):
        peer = row_peers[d]
        return pltpu.make_async_remote_copy(
            src_ref=grad_send.at[c, peer[0]],
            dst_ref=grad_recv.at[c, d],
            send_sem=grad_ssem.at[c, d],
            recv_sem=grad_rsem.at[c, d],
            device_id=peer,
            device_id_type=pl.DeviceIdType.MESH,
        )

    for c in range(chunks):
        part = jnp.dot(
            all_signals, a_block[:, c * chunk : (c + 1) * chunk], preferred_element_type=F32
        ).astype(BF16)
        for k in range(rows):
            grad_send[c, k] = part[k * group : (k + 1) * group, :]
        for d in range(rows - 1):
            grad_copy(c, d).start()

    pl.when(jnp.logical_not(on_diagonal))(move.wait_recv)
    moved = split3(moved_recv[...])
    for c in range(chunks):
        span = slice(c * chunk, (c + 1) * chunk)
        before = add3(
            jnp.dot(
                moved,
                one_hot(index_own[steps - 2], c * chunk, chunk).astype(BF16),
                preferred_element_type=F32,
            )
        )
        mask = jnp.sum(one_hot(index_own[steps - 1], c * chunk, chunk), axis=0, keepdims=True)
        gradient = grad_send[c, i].astype(F32)
        for d in range(rows - 1):
            grad_copy(c, d).wait_recv()
            gradient += grad_recv[c, d].astype(F32)
        stepped = before + STEP_SIZE * gradient
        estimate[:, span] = stepped * mask
        norm_all[i, :, span] = jnp.sum(stepped * stepped, axis=0, keepdims=True)

    copies = [remote(norm_all.at[i], norm_all.at[i], peer, next(sems)) for peer in row_peers]
    for copy in copies:
        copy.start()
    for copy in copies:
        copy.wait_recv()
    pending += copies
    summed = jnp.sum(norm_all[...], axis=0)
    norms[...] = jnp.sqrt(summed[:, :width])
    energies[...] = summed[:, width:] / total_count

    for other, copy in first_copies:
        pl.when(other)(copy.wait_send)
    pl.when(jnp.logical_not(on_diagonal))(move.wait_send)
    for copy in pending:
        copy.wait_send()
    for c in range(chunks):
        for d in range(rows - 1):
            grad_copy(c, d).wait_send()


def solution(mesh, far=4, high=4, chunk=512):
    rows = mesh.shape["row"]

    def local(matrix, measured, support):
        depth, width = matrix.shape
        signals = measured.shape[0]
        group = signals // rows
        steps = support.shape[0]
        turns = steps - 1
        span = min(chunk, width)
        chunks = width // span
        estimate, norms, energies = pl.pallas_call(
            functools.partial(
                kernel, (rows, far, high, float(signals * depth * rows))
            ),
            out_shape=(
                jax.ShapeDtypeStruct((group, width), F32),
                jax.ShapeDtypeStruct((1, width), F32),
                jax.ShapeDtypeStruct((1, KMAX), F32),
            ),
            in_specs=[
                pl.BlockSpec(memory_space=pltpu.VMEM),
                pl.BlockSpec(memory_space=pltpu.VMEM),
                pl.BlockSpec(memory_space=pl.ANY),
            ],
            out_specs=(pl.BlockSpec(memory_space=pltpu.VMEM),) * 3,
            scratch_shapes=[
                pltpu.VMEM((depth, width), BF16),
                pltpu.VMEM((steps, KMAX, 1), jnp.int32),
                pltpu.VMEM((turns, KMAX, 1), jnp.int32),
                pltpu.VMEM((turns * KMAX, depth), F32),
                pltpu.VMEM((turns, rows, KMAX, depth), BF16),
                pltpu.VMEM((rows, group, KMAX), BF16),
                pltpu.VMEM((rows, group, KMAX), BF16),
                pltpu.VMEM((turns, rows, group, KMAX), BF16),
                pltpu.VMEM((turns, rows - 1, group, KMAX), BF16),
                pltpu.VMEM((turns, rows, group, KMAX), BF16),
                pltpu.VMEM((group, KMAX), F32),
                pltpu.VMEM((turns, high, group, depth), BF16),
                pltpu.VMEM((group, KMAX), F32),
                pltpu.VMEM((group, KMAX), F32),
                pltpu.VMEM((rows, group + 16, depth), BF16),
                pltpu.VMEM((chunks, rows, group, span), BF16),
                pltpu.VMEM((chunks, rows - 1, group, span), BF16),
                pltpu.VMEM((rows, 1, width + KMAX), F32),
                pltpu.SemaphoreType.DMA((chunks,)),
                pltpu.SemaphoreType.DMA((120,)),
                pltpu.SemaphoreType.DMA((120,)),
                pltpu.SemaphoreType.DMA((chunks, rows - 1)),
                pltpu.SemaphoreType.DMA((chunks, rows - 1)),
            ],
            compiler_params=pltpu.CompilerParams(
                collective_id=0, has_side_effects=True, vmem_limit_bytes=56 * 2**20
            ),
        )(support, measured, matrix)
        return estimate, norms.reshape(width), energies[0, :steps]

    return jax.shard_map(
        local,
        mesh=mesh,
        in_specs=(P("row", "col"), P(None, "row"), P()),
        out_specs=(P("row", "col"), P("col"), P()),
        check_vma=False,
    )
```

```python
import functools

import jax
import jax.numpy as jnp
from jax import lax
from jax.experimental import pallas as pl
from jax.experimental.pallas import tpu as pltpu
from jax.sharding import PartitionSpec as P

KMAX = 128
STEP_SIZE = 0.25
CORES = 2
NEAR = (((1,), (1,)), ((), ()))
F32 = jnp.float32
BF16 = jnp.bfloat16


def iota(shape, dim):
    return lax.broadcasted_iota(jnp.int32, shape, dim)


def window(line, start, width):
    count = line.shape[1]
    below = jnp.sum(jnp.where(line < start, 1.0, 0.0), axis=1, keepdims=True)
    upto = jnp.sum(jnp.where(line < start + width, 1.0, 0.0), axis=1, keepdims=True)
    place = iota((KMAX, count), 1) - iota((KMAX, count), 0)
    local = (line - start).astype(F32)
    found = jnp.sum(
        jnp.where(place == below.astype(jnp.int32), local, 0.0), axis=1, keepdims=True
    )
    there = iota((KMAX, 1), 0).astype(F32) < upto - below
    return jnp.where(there, found, -1.0).astype(jnp.int32)


def one_hot(index, first, width):
    return jnp.where(iota((KMAX, width), 1) + first == index, 1.0, 0.0)


def split3(value):
    high = value.astype(BF16)
    rest = value - high.astype(F32)
    middle = rest.astype(BF16)
    low = (rest - middle.astype(F32)).astype(BF16)
    return jnp.concatenate([high, middle, low], axis=0)


def add3(value):
    third = value.shape[0] // 3
    return value[:third] + value[third : 2 * third] + value[2 * third :]


def kernel(
    shape,
    support_in,
    measured_in,
    matrix,
    kept_out,
    sums_out,
    support,
    measured,
    a_block,
    index_own,
    index_held,
    image,
    kept,
    first_send,
    first_recv,
    slope_send,
    slope_recv,
    current_all,
    held,
    seen_all,
    moved_send,
    moved_recv,
    residual_all,
    grad_send,
    by_x,
    by_z,
    pair_send,
    pair_recv,
    line_send,
    line_recv,
    norm_all,
    load_sem,
    send_sem,
    recv_sem,
):
    rows, far, high, along_x = shape
    pairs = rows // 2
    depth, width = matrix.shape
    group = measured.shape[0] // rows
    steps = support.shape[0]
    chunk = grad_send.shape[3]
    chunks = width // chunk
    i = lax.axis_index("row")
    col = lax.axis_index("col")
    x = lax.rem(i, pairs)
    z = i // pairs
    core = lax.rem(col, CORES)
    h = lax.rem(col // CORES, high)
    y = col // (CORES * high)
    q = y * CORES + core
    sending = iter(range(send_sem.shape[0]))
    landing = iter(range(recv_sem.shape[0]))
    sent = []

    def at(yy, hh, cc):
        return (yy * high + hh) * CORES + cc

    def member(k):
        return at(k // CORES, h, lax.rem(k, CORES))

    def far_first(count):
        return sorted(range(1, count), key=lambda d: -min(d, count - d))

    def remote(src, dst, where, out, back):
        return pltpu.make_async_remote_copy(
            src_ref=src,
            dst_ref=dst,
            send_sem=send_sem.at[out],
            recv_sem=recv_sem.at[back],
            device_id=where,
            device_id_type=pl.DeviceIdType.MESH,
        )

    def await_all(sems, slot, ref):
        pltpu.make_async_copy(ref, ref, sems.at[slot]).wait()

    x_shift = far_first(pairs)
    offsets = [(1, d) for d in x_shift] + [(0, d) for d in x_shift] + [(1, 0)]
    row_peers = [
        (lax.rem(z + dz, 2) * pairs + lax.rem(x + dx, pairs), col) for dz, dx in offsets
    ]
    x_peers = [(z * pairs + lax.rem(x + d, pairs), col) for d in x_shift]
    across = ((1 - z) * pairs + x, col)
    y_shift = far_first(far)
    y_peers = [(i, at(lax.rem(y + d, far), h, core)) for d in y_shift]
    y_from = [lax.rem(y - d + far, far) for d in y_shift]
    h_peers = [(i, at(y, lax.rem(h + d, high), core)) for d in far_first(high)]
    partner = (i, at(y, h, 1 - core))

    barrier = pltpu.get_barrier_semaphore()
    for peer in row_peers + y_peers + h_peers + [partner]:
        pl.semaphore_signal(
            barrier, inc=1, device_id=peer, device_id_type=pl.DeviceIdType.MESH
        )
    on_diagonal = i == q
    off_diagonal = jnp.logical_not(on_diagonal)
    for k in range(rows):

        @pl.when(jnp.logical_or(off_diagonal, i != k))
        def _():
            pl.semaphore_signal(
                barrier,
                inc=1,
                device_id=(k, member(i)),
                device_id_type=pl.DeviceIdType.MESH,
            )

    support_load = pltpu.make_async_copy(support_in, support, load_sem.at[chunks])
    support_load.start()
    loads = [
        pltpu.make_async_copy(
            matrix.at[:, pl.ds(c * chunk, chunk)],
            a_block.at[:, pl.ds(c * chunk, chunk)],
            load_sem.at[c],
        )
        for c in range(chunks)
    ]
    for load in loads:
        load.start()
    measured_load = pltpu.make_async_copy(measured_in, measured, load_sem.at[chunks + 1])
    measured_load.start()
    support_load.wait()

    def find_own(t):
        index_own[t] = window(support[t : t + 1, :], col * width, width)

    def pick(first, last, loaded):
        total = jnp.zeros(((last - first) * KMAX, depth), F32)
        for c in range(chunks):
            if not loaded:
                loads[c].wait()
            hot = jnp.concatenate(
                [one_hot(index_own[t], c * chunk, chunk).astype(BF16) for t in range(first, last)],
                axis=0,
            )
            total += lax.dot_general(
                hot, a_block[:, c * chunk : (c + 1) * chunk], NEAR, preferred_element_type=F32
            )
        for t in range(first, last):
            kept[t, q] = total[(t - first) * KMAX : (t - first + 1) * KMAX, :].astype(BF16)

    find_own(0)
    pick(0, 1, False)
    measured_load.wait()

    first = lax.dot_general(
        measured[...].astype(BF16), kept[0, q], NEAR, preferred_element_type=F32
    ).astype(BF16)
    for k in range(rows):
        first_send[k] = first[k * group : (k + 1) * group, :]

    pl.semaphore_wait(
        barrier,
        len(row_peers + y_peers + h_peers) + 1 + rows - jnp.where(on_diagonal, 1, 0),
    )

    first_out, first_back = next(sending), next(landing)
    for k in range(rows):
        copy = remote(
            first_send.at[k], first_recv.at[i], (q, member(k)), first_out, first_back
        )
        other = jnp.logical_or(off_diagonal, q != k)
        pl.when(other)(copy.start)

        @pl.when(jnp.logical_not(other))
        def _():
            first_recv[i] = first_send[k]

    def spread(buffer):
        own = buffer.at[q]
        out, back = next(sending), next(landing)
        to_y = [remote(own, own, peer, out, next(landing)) for peer in y_peers]
        for copy in to_y:
            copy.start()
        remote(own, own, partner, out, back).start()
        sent.append((out, buffer.at[pl.ds(0, rows - 1)]))
        return to_y, out, back

    def relay(buffer, parts):
        to_y, out, back = parts
        for n, copy in enumerate(to_y):
            copy.wait_recv()
            slot = buffer.at[y_from[n] * CORES + core]
            remote(slot, slot, partner, out, back).start()

    def relayed(buffer, parts):
        await_all(recv_sem, parts[2], buffer.at[pl.ds(0, far)])

    spreads = [spread(kept.at[0])]
    for t in range(1, steps - 1):
        find_own(t)
    pick(1, steps - 1, True)
    for t in range(1, steps - 1):
        spreads.append(spread(kept.at[t]))

    for t in range(steps - 1):
        index_held[t] = window(support[t : t + 1, :], member(i) * width, width)
    find_own(steps - 1)

    def carried(t, value):
        diagonal = iota((KMAX, KMAX), 0) == iota((KMAX, KMAX), 1)
        after = jnp.sum(
            jnp.where(diagonal, index_held[t + 1].astype(F32), 0.0), axis=0, keepdims=True
        ).astype(jnp.int32)
        before = index_held[t]
        same = jnp.where(jnp.logical_and(before == after, before >= 0), 1.0, 0.0).astype(BF16)
        return add3(jnp.dot(split3(value), same, preferred_element_type=F32))

    pl.when(on_diagonal)(
        lambda: await_all(recv_sem, first_back, first_recv.at[pl.ds(0, rows - 1)])
    )
    pl.when(off_diagonal)(lambda: await_all(recv_sem, first_back, first_recv))
    current = STEP_SIZE * jnp.sum(first_recv[...].astype(F32), axis=0)

    own_measured = measured[pl.ds(pl.multiple_of(q * group, group), group), :]
    energy = [jnp.sum(own_measured * own_measured)]
    for t in range(steps - 1):
        if t > 0:
            relayed(kept.at[t], spreads[t])
            slope = lax.dot_general(
                residual.astype(BF16),
                kept[t].reshape(rows * KMAX, depth),
                NEAR,
                preferred_element_type=F32,
            ).astype(BF16)
            for k in range(rows):
                slope_send[t - 1, k] = slope[:, k * KMAX : (k + 1) * KMAX]
            out, back = next(sending), next(landing)
            for n, peer in enumerate(row_peers):
                remote(
                    slope_send.at[t - 1, peer[0]], slope_recv.at[t - 1, n], peer, out, back
                ).start()
            sent.append((out, slope_recv.at[t - 1]))
            carry = carried(t - 1, held[...])
            await_all(recv_sem, back, slope_recv.at[t - 1])
            gathered = slope_send[t - 1, i].astype(F32) + jnp.sum(
                slope_recv[t - 1].astype(F32), axis=0
            )
            current = carry + STEP_SIZE * gathered
        held[...] = current
        current_all[t, i] = current.astype(BF16)
        out, back = next(sending), next(landing)
        mine = current_all.at[t, i]
        for peer in row_peers:
            remote(mine, mine, peer, out, back).start()
        others = current_all.at[t, pl.ds(0, rows - 1)]
        sent.append((out, others))
        if t == steps - 2:
            moved_send[...] = current
            move = remote(moved_send, moved_recv, (q, member(i)), next(sending), next(landing))
            pl.when(off_diagonal)(move.start)

            @pl.when(on_diagonal)
            def _():
                moved_recv[...] = moved_send[...]

        if t != 1:
            following = t if t == 0 else None
            if following is not None:
                relay(kept.at[0], spreads[0])
                relayed(kept.at[0], spreads[0])
        elif steps > 3:
            relay(kept.at[2], spreads[2])
        await_all(recv_sem, back, others)
        signals = jnp.concatenate([current_all[t, k] for k in range(rows)], axis=1)
        seen_all[t, h] = jnp.dot(
            signals, kept[t].reshape(rows * KMAX, depth), preferred_element_type=F32
        ).astype(BF16)
        out, back = next(sending), next(landing)
        mine = seen_all.at[t, h]
        for peer in h_peers:
            remote(mine, mine, peer, out, back).start()
        others = seen_all.at[t, pl.ds(0, high - 1)]
        sent.append((out, others))
        if t == 0:
            relay(kept.at[1], spreads[1])
        await_all(recv_sem, back, others)
        residual = own_measured - jnp.sum(seen_all[t].astype(F32), axis=0)
        energy.append(jnp.sum(residual * residual))

    lanes = iota((16, depth), 1)
    values = jnp.zeros((16, depth), F32)
    for t in range(steps):
        values = jnp.where(lanes == t, energy[t], values)
    top = values.astype(BF16).astype(F32)
    mid = (values - top).astype(BF16).astype(F32)
    low = values - top - mid
    line = iota((16, depth), 0)
    values = jnp.where(line == 0, top, jnp.where(line == 1, mid, jnp.where(line == 2, low, 0.0)))
    residual_all[q] = jnp.concatenate([residual.astype(BF16), values.astype(BF16)], axis=0)
    parts = spread(residual_all)
    relay(residual_all, parts)
    relayed(residual_all, parts)

    all_signals = jnp.concatenate([residual_all[k, :group, :] for k in range(rows)], axis=0)
    first_by_x = list(range(along_x))
    z_out, x_out = next(sending), next(sending)
    arrive = [next(landing) for _ in range(chunks)]
    across_first = list(range(along_x, chunks))
    order = []
    for n in range(max(len(first_by_x), len(across_first))):
        order += across_first[n : n + 1] + first_by_x[n : n + 1]
    for c in order:
        part = jnp.dot(
            all_signals, a_block[:, c * chunk : (c + 1) * chunk], preferred_element_type=F32
        ).astype(BF16)
        if c < along_x:
            for k in range(rows):
                grad_send[c, k % pairs * 2 + k // pairs] = part[k * group : (k + 1) * group, :]
            for n, peer in enumerate(x_peers):
                remote(
                    grad_send.at[c, pl.ds(lax.rem(peer[0], pairs) * 2, 2)],
                    by_x.at[c, n],
                    peer,
                    x_out,
                    arrive[c],
                ).start()
        else:
            for k in range(rows):
                grad_send[c, k] = part[k * group : (k + 1) * group, :]
            remote(
                grad_send.at[c, pl.ds((1 - z) * pairs, pairs)],
                by_z.at[c - along_x],
                across,
                z_out,
                arrive[c],
            ).start()
    sent.append((x_out, by_x))
    sent.append((z_out, by_z))
    second = {}
    pair_out, line_out = next(sending), next(sending)
    for c in order:
        second[c] = next(landing)
        if c < along_x:
            await_all(recv_sem, arrive[c], by_x.at[c])
            total = grad_send[c, pl.ds(x * 2, 2)].astype(F32)
            for n in range(pairs - 1):
                total += by_x[c, n].astype(F32)
            pair_send[c] = total.astype(BF16)
            remote(
                pair_send.at[c, 1 - z], pair_recv.at[c], across, pair_out, second[c]
            ).start()
        else:
            n = c - along_x
            await_all(recv_sem, arrive[c], by_z.at[n])
            total = grad_send[c, pl.ds(z * pairs, pairs)].astype(F32) + by_z[n].astype(F32)
            line_send[n] = total.astype(BF16)
            for m, peer in enumerate(x_peers):
                remote(
                    line_send.at[n, lax.rem(peer[0], pairs)],
                    line_recv.at[n, m],
                    peer,
                    line_out,
                    second[c],
                ).start()
    sent.append((pair_out, pair_recv))
    sent.append((line_out, line_recv))

    norm_all[i, :, width:] = jnp.sum(
        jnp.sum(residual_all[:, group:, :KMAX].astype(F32), axis=0), axis=0, keepdims=True
    )
    pl.when(off_diagonal)(move.wait_recv)
    moved = split3(moved_recv[...])
    for c in order:
        span = slice(c * chunk, (c + 1) * chunk)
        before = add3(
            jnp.dot(
                moved,
                one_hot(index_own[steps - 2], c * chunk, chunk).astype(BF16),
                preferred_element_type=F32,
            )
        )
        mask = jnp.sum(one_hot(index_own[steps - 1], c * chunk, chunk), axis=0, keepdims=True)
        if c < along_x:
            await_all(recv_sem, second[c], pair_recv.at[c])
            gradient = pair_send[c, z].astype(F32) + pair_recv[c].astype(F32)
        else:
            n = c - along_x
            await_all(recv_sem, second[c], line_recv.at[n])
            gradient = line_send[n, x].astype(F32) + jnp.sum(line_recv[n].astype(F32), axis=0)
        stepped = before + STEP_SIZE * gradient
        kept_out[:, span] = stepped * mask
        norm_all[i, :, span] = jnp.sum(stepped * stepped, axis=0, keepdims=True)

    out, back = next(sending), next(landing)
    mine = norm_all.at[i]
    for peer in row_peers:
        remote(mine, mine, peer, out, back).start()
    others = norm_all.at[pl.ds(0, rows - 1)]
    sent.append((out, others))
    await_all(recv_sem, back, others)
    sums_out[...] = jnp.sum(norm_all[...], axis=0)

    pl.when(on_diagonal)(
        lambda: await_all(send_sem, first_out, first_send.at[pl.ds(0, rows - 1)])
    )
    pl.when(off_diagonal)(lambda: await_all(send_sem, first_out, first_send))
    pl.when(off_diagonal)(move.wait_send)
    for out, ref in sent:
        await_all(send_sem, out, ref)


def finish(total_count, kept, sums, estimate, norms, energies):
    width = kept.shape[1]
    estimate[...] = kept[...]
    norms[...] = jnp.sqrt(sums[:, :width]).reshape(width)
    for t in range(energies.shape[0]):
        energies[t] = sums[0, width + t] / total_count


def solution(mesh, far=4, high=4, chunk=512, along_x=4):
    rows = mesh.shape["row"]

    def local(matrix, measured, support):
        depth, width = matrix.shape
        signals = measured.shape[0]
        group = signals // rows
        pairs = rows // 2
        steps = support.shape[0]
        turns = steps - 1
        span = min(chunk, width)
        chunks = width // span
        along_z = chunks - along_x
        in_vmem = pl.BlockSpec(memory_space=pltpu.VMEM)
        in_hbm = pl.BlockSpec(memory_space=pltpu.HBM)
        kept, sums = pl.pallas_call(
            functools.partial(kernel, (rows, far, high, along_x)),
            out_shape=(
                jax.ShapeDtypeStruct((group, width), F32),
                jax.ShapeDtypeStruct((1, width + KMAX), F32),
            ),
            in_specs=[in_hbm] * 3,
            out_specs=(in_vmem,) * 2,
            scratch_shapes=[
                pltpu.VMEM(support.shape, jnp.int32),
                pltpu.VMEM(measured.shape, F32),
                pltpu.VMEM((depth, width), BF16),
                pltpu.VMEM((steps, KMAX, 1), jnp.int32),
                pltpu.VMEM((turns, KMAX, 1), jnp.int32),
                pltpu.VMEM((turns * KMAX, depth), F32),
                pltpu.VMEM((turns, rows, KMAX, depth), BF16),
                pltpu.VMEM((rows, group, KMAX), BF16),
                pltpu.VMEM((rows, group, KMAX), BF16),
                pltpu.VMEM((turns, rows, group, KMAX), BF16),
                pltpu.VMEM((turns, rows - 1, group, KMAX), BF16),
                pltpu.VMEM((turns, rows, group, KMAX), BF16),
                pltpu.VMEM((group, KMAX), F32),
                pltpu.VMEM((turns, high, group, depth), BF16),
                pltpu.VMEM((group, KMAX), F32),
                pltpu.VMEM((group, KMAX), F32),
                pltpu.VMEM((rows, group + 16, depth), BF16),
                pltpu.VMEM((chunks, rows, group, span), BF16),
                pltpu.VMEM((along_x, pairs - 1, 2, group, span), BF16),
                pltpu.VMEM((along_z, pairs, group, span), BF16),
                pltpu.VMEM((along_x, 2, group, span), BF16),
                pltpu.VMEM((along_x, group, span), BF16),
                pltpu.VMEM((along_z, pairs, group, span), BF16),
                pltpu.VMEM((along_z, pairs - 1, group, span), BF16),
                pltpu.VMEM((rows, 1, width + KMAX), F32),
                pltpu.SemaphoreType.DMA((chunks + 2,)),
                pltpu.SemaphoreType.DMA((19,)),
                pltpu.SemaphoreType.DMA((28 + 2 * chunks,)),
            ],
            compiler_params=pltpu.CompilerParams(
                collective_id=0, has_side_effects=True, vmem_limit_bytes=40 * 2**20
            ),
        )(*(pltpu.with_memory_space_constraint(a, pltpu.HBM) for a in (support, measured, matrix)))
        return pl.pallas_call(
            functools.partial(finish, float(signals * depth * rows)),
            out_shape=(
                jax.ShapeDtypeStruct((group, width), F32),
                jax.ShapeDtypeStruct((width,), F32),
                jax.ShapeDtypeStruct((steps,), F32),
            ),
            in_specs=[in_vmem] * 2,
            out_specs=(in_vmem, in_vmem, pl.BlockSpec(memory_space=pltpu.SMEM)),
            compiler_params=pltpu.CompilerParams(vmem_limit_bytes=4 * 2**20),
        )(kept, sums)

    return jax.shard_map(
        local,
        mesh=mesh,
        in_specs=(P("row", "col"), P(None, "row"), P()),
        out_specs=(P("row", "col"), P("col"), P()),
        check_vma=False,
    )
```

```python
import functools

import jax
import jax.numpy as jnp
from jax import lax
from jax.experimental import pallas as pl
from jax.experimental.pallas import tpu as pltpu
from jax.sharding import PartitionSpec as P

KMAX = 128
STEP_SIZE = 0.25
CORES = 2
LEAD = 1
NEAR = (((1,), (1,)), ((), ()))
F32 = jnp.float32
BF16 = jnp.bfloat16


def iota(shape, dim):
    return lax.broadcasted_iota(jnp.int32, shape, dim)


def window(line, start, width):
    count = line.shape[1]
    below = jnp.sum(jnp.where(line < start, 1.0, 0.0), axis=1, keepdims=True)
    upto = jnp.sum(jnp.where(line < start + width, 1.0, 0.0), axis=1, keepdims=True)
    place = iota((KMAX, count), 1) - iota((KMAX, count), 0)
    local = (line - start).astype(F32)
    found = jnp.sum(
        jnp.where(place == below.astype(jnp.int32), local, 0.0), axis=1, keepdims=True
    )
    there = iota((KMAX, 1), 0).astype(F32) < upto - below
    return jnp.where(there, found, -1.0).astype(jnp.int32)


def one_hot(index, first, width):
    return jnp.where(iota((KMAX, width), 1) + first == index, 1.0, 0.0)


def split3(value):
    high = value.astype(BF16)
    rest = value - high.astype(F32)
    middle = rest.astype(BF16)
    low = (rest - middle.astype(F32)).astype(BF16)
    return jnp.concatenate([high, middle, low], axis=0)


def add3(value):
    third = value.shape[0] // 3
    return value[:third] + value[third : 2 * third] + value[2 * third :]


def kernel(
    shape,
    support_in,
    measured_in,
    matrix,
    kept_out,
    sums_out,
    support,
    measured,
    a_block,
    index_own,
    index_held,
    kept,
    first_send,
    first_recv,
    slope_send,
    slope_recv,
    current_all,
    held,
    seen_all,
    moved_send,
    moved_recv,
    residual_all,
    energy_all,
    energy_sum,
    grad_send,
    by_x,
    by_z,
    pair_send,
    pair_recv,
    line_send,
    line_recv,
    norm_all,
    load_sem,
    send_sem,
    recv_sem,
):
    rows, far, high, along_x = shape
    pairs = rows // 2
    depth, width = matrix.shape
    group = measured.shape[0] // rows
    party = CORES * group
    steps = support.shape[0]
    chunk = grad_send.shape[3]
    chunks = width // chunk
    i = lax.axis_index("row")
    col = lax.axis_index("col")
    x = lax.rem(i, pairs)
    z = i // pairs
    core = lax.rem(col, CORES)
    h = lax.rem(col // CORES, high)
    y = col // (CORES * high)
    q = y * CORES + core
    lead = core == LEAD
    follow = core != LEAD
    sending = iter(range(send_sem.shape[0]))
    landing = iter(range(recv_sem.shape[0]))
    sent = []
    lead_sent = []

    def at(yy, hh, cc):
        return (yy * high + hh) * CORES + cc

    def member(k):
        return at(k // CORES, h, lax.rem(k, CORES))

    def far_first(count):
        return sorted(range(1, count), key=lambda d: -min(d, count - d))

    def remote(src, dst, where, out, back):
        return pltpu.make_async_remote_copy(
            src_ref=src,
            dst_ref=dst,
            send_sem=send_sem.at[out],
            recv_sem=recv_sem.at[back],
            device_id=where,
            device_id_type=pl.DeviceIdType.MESH,
        )

    def await_all(sems, slot, ref):
        pltpu.make_async_copy(ref, ref, sems.at[slot]).wait()

    x_shift = far_first(pairs)
    offsets = [(1, d) for d in x_shift] + [(0, d) for d in x_shift] + [(1, 0)]
    row_peers = [
        (lax.rem(z + dz, 2) * pairs + lax.rem(x + dx, pairs), col) for dz, dx in offsets
    ]
    x_peers = [(z * pairs + lax.rem(x + d, pairs), col) for d in x_shift]
    across = ((1 - z) * pairs + x, col)
    y_shift = far_first(far)
    y_near = [lax.rem(y + d, far) for d in y_shift]
    y_from = [lax.rem(y - d + far, far) for d in y_shift]
    y_leads = [(i, at(yy, h, LEAD)) for yy in y_near]
    h_peers = [(i, at(y, lax.rem(h + d, high), core)) for d in far_first(high)]
    partner = (i, at(y, h, 1 - core))
    holder = (q, at(i // CORES, h, LEAD))

    support_load = pltpu.make_async_copy(support_in, support, load_sem.at[chunks])
    support_load.start()
    barrier = pltpu.get_barrier_semaphore()

    def greet(peer):
        pl.semaphore_signal(
            barrier, inc=1, device_id=peer, device_id_type=pl.DeviceIdType.MESH
        )

    on_diagonal = i == q
    loop = jnp.logical_and(on_diagonal, lead)
    no_loop = jnp.logical_not(loop)
    pl.when(no_loop)(lambda: greet(holder))
    for peer in row_peers + [partner]:
        greet(peer)

    @pl.when(lead)
    def _():
        for k in range(rows):
            pl.when(jnp.logical_or(jnp.logical_not(on_diagonal), i != k))(
                lambda k=k: greet((k, member(i)))
            )
        for yy in y_near:
            for cc in range(CORES):
                greet((i, at(yy, h, cc)))
        for peer in h_peers:
            greet(peer)

    greetings = (
        len(row_peers) + 1 + len(y_leads) + far
        + jnp.where(lead, len(h_peers) + CORES, 0)
        - jnp.where(loop, 2, 0)
    )

    loads = [
        pltpu.make_async_copy(
            matrix.at[:, pl.ds(c * chunk, chunk)],
            a_block.at[:, pl.ds(c * chunk, chunk)],
            load_sem.at[c],
        )
        for c in range(chunks)
    ]
    for load in loads:
        load.start()
    measured_load = pltpu.make_async_copy(measured_in, measured, load_sem.at[chunks + 1])
    measured_load.start()
    support_load.wait()

    def find_own(t):
        index_own[t] = window(support[t : t + 1, :], col * width, width)

    def pick(first, last, loaded):
        total = jnp.zeros(((last - first) * KMAX, depth), F32)
        for c in range(chunks):
            if not loaded:
                loads[c].wait()
            hot = jnp.concatenate(
                [one_hot(index_own[t], c * chunk, chunk).astype(BF16) for t in range(first, last)],
                axis=0,
            )
            total += lax.dot_general(
                hot, a_block[:, c * chunk : (c + 1) * chunk], NEAR, preferred_element_type=F32
            )
        for t in range(first, last):
            kept[t, q] = total[(t - first) * KMAX : (t - first + 1) * KMAX, :].astype(BF16)

    find_own(0)
    pick(0, 1, False)
    measured_load.wait()

    first = lax.dot_general(
        measured[...].astype(BF16), kept[0, q], NEAR, preferred_element_type=F32
    ).astype(BF16)
    for k in range(far):
        first_send[k] = first[k * party : (k + 1) * party, :]

    pl.semaphore_wait(barrier, greetings)

    first_out, first_back = next(sending), next(landing)
    for k in range(far):
        copy = remote(
            first_send.at[k], first_recv.at[i], (q, at(k, h, LEAD)), first_out, first_back
        )
        other = jnp.logical_or(no_loop, y != k)
        pl.when(other)(copy.start)

        @pl.when(jnp.logical_not(other))
        def _():
            first_recv[i] = first_send[k]

    kept_out_sem = [next(sending) for _ in range(steps - 1)]
    kept_back = [next(landing) for _ in range(steps - 1)]

    def spread(t):
        own = kept.at[t, q]
        for peer in y_leads:
            remote(own, own, peer, kept_out_sem[t], kept_back[t]).start()
        pl.when(follow)(remote(own, own, partner, kept_out_sem[t], kept_back[t]).start)

    spread(0)
    for t in range(1, steps - 1):
        find_own(t)
    pick(1, steps - 1, True)
    for t in range(1, steps - 1):
        spread(t)
    find_own(steps - 1)

    def carried(t, value):
        diagonal = iota((KMAX, KMAX), 0) == iota((KMAX, KMAX), 1)
        after = jnp.sum(
            jnp.where(diagonal, index_held[t + 1].astype(F32), 0.0), axis=0, keepdims=True
        ).astype(jnp.int32)
        before = index_held[t]
        same = jnp.where(jnp.logical_and(before == after, before >= 0), 1.0, 0.0).astype(BF16)
        return add3(jnp.dot(split3(value), same, preferred_element_type=F32))

    move_out, move_back = next(sending), next(landing)
    energy_out, energy_back, total_out, total_back = (
        next(sending), next(landing), next(sending), next(landing)
    )
    r_out, r_back, pass_out, pass_back = (
        next(sending), [next(landing) for _ in y_leads], next(sending), next(landing)
    )
    moves = [
        remote(moved_send.at[n], moved_recv, (CORES * y + n, member(i)), move_out, move_back)
        for n in range(CORES)
    ]
    here = [jnp.logical_and(on_diagonal, core == n) for n in range(CORES)]

    @pl.when(lead)
    def _():
        for t in range(steps - 1):
            index_held[t] = window(support[t : t + 1, :], member(i) * width, width)
        pl.when(on_diagonal)(
            lambda: await_all(recv_sem, first_back, first_recv.at[pl.ds(0, rows - 1)])
        )
        pl.when(jnp.logical_not(on_diagonal))(lambda: await_all(recv_sem, first_back, first_recv))
        current = STEP_SIZE * jnp.sum(first_recv[...].astype(F32), axis=0)

        own_measured = measured[pl.ds(pl.multiple_of(y * party, party), party), :]
        energy = [jnp.sum(own_measured * own_measured)]
        for t in range(steps - 1):
            if t > 0:
                await_all(recv_sem, kept_back[t], kept.at[t, pl.ds(0, rows - 1)])
                slope = lax.dot_general(
                    residual.astype(BF16),
                    kept[t].reshape(rows * KMAX, depth),
                    NEAR,
                    preferred_element_type=F32,
                ).astype(BF16)
                for k in range(rows):
                    slope_send[t - 1, k] = slope[:, k * KMAX : (k + 1) * KMAX]
                out, back = next(sending), next(landing)
                for n, peer in enumerate(row_peers):
                    remote(
                        slope_send.at[t - 1, peer[0]], slope_recv.at[t - 1, n], peer, out, back
                    ).start()
                lead_sent.append((out, lambda t=t: slope_recv.at[t - 1]))
                carry = carried(t - 1, held[...])
                await_all(recv_sem, back, slope_recv.at[t - 1])
                gathered = slope_send[t - 1, i].astype(F32) + jnp.sum(
                    slope_recv[t - 1].astype(F32), axis=0
                )
                current = carry + STEP_SIZE * gathered
            held[...] = current
            current_all[t, i] = current.astype(BF16)
            out, back = next(sending), next(landing)
            mine = current_all.at[t, i]
            for peer in row_peers:
                remote(mine, mine, peer, out, back).start()
            others = current_all.at[t, pl.ds(0, rows - 1)]
            lead_sent.append((out, lambda t=t: current_all.at[t, pl.ds(0, rows - 1)]))
            if t == steps - 2:
                for n in range(CORES):
                    moved_send[n] = current[n * group : (n + 1) * group, :]
                    pl.when(jnp.logical_not(here[n]))(moves[n].start)

                    @pl.when(here[n])
                    def _():
                        moved_recv[...] = moved_send[n]

            if t == 0:
                await_all(recv_sem, kept_back[t], kept.at[t, pl.ds(0, rows - 1)])
            await_all(recv_sem, back, others)
            signals = jnp.concatenate([current_all[t, k] for k in range(rows)], axis=1)
            seen_all[t, h] = jnp.dot(
                signals, kept[t].reshape(rows * KMAX, depth), preferred_element_type=F32
            ).astype(BF16)
            out, back = next(sending), next(landing)
            mine = seen_all.at[t, h]
            for peer in h_peers:
                remote(mine, mine, peer, out, back).start()
            others = seen_all.at[t, pl.ds(0, high - 1)]
            lead_sent.append((out, lambda t=t: seen_all.at[t, pl.ds(0, high - 1)]))
            await_all(recv_sem, back, others)
            residual = own_measured - jnp.sum(seen_all[t].astype(F32), axis=0)
            energy.append(jnp.sum(residual * residual))

        residual_all[y] = residual.astype(BF16)
        own = residual_all.at[y]
        copies = [remote(own, own, peer, r_out, r_back[n]) for n, peer in enumerate(y_leads)]
        for copy in copies:
            copy.start()
        remote(own, own, partner, pass_out, pass_back).start()
        lanes = iota((1, KMAX), 1)
        values = jnp.zeros((1, KMAX), F32)
        for t in range(steps):
            values = jnp.where(lanes == t, energy[t], values)
        energy_all[y] = values
        mine = energy_all.at[y]
        for peer in y_leads:
            remote(mine, mine, peer, energy_out, energy_back).start()
        for n, copy in enumerate(copies):
            copy.wait_recv()
            slot = residual_all.at[y_from[n]]
            remote(slot, slot, partner, pass_out, pass_back).start()
        lead_sent.append((r_out, lambda: residual_all.at[pl.ds(0, far - 1)]))
        lead_sent.append((pass_out, lambda: residual_all))
        lead_sent.append((energy_out, lambda: energy_all.at[pl.ds(0, far - 1)]))

    pl.when(follow)(lambda: await_all(recv_sem, pass_back, residual_all))

    all_signals = jnp.concatenate([residual_all[k] for k in range(far)], axis=0)
    first_by_x = list(range(along_x))
    z_out, x_out = next(sending), next(sending)
    arrive = [next(landing) for _ in range(chunks)]
    across_first = list(range(along_x, chunks))
    order = []
    for n in range(max(len(first_by_x), len(across_first))):
        order += across_first[n : n + 1] + first_by_x[n : n + 1]
    for c in order:
        part = jnp.dot(
            all_signals, a_block[:, c * chunk : (c + 1) * chunk], preferred_element_type=F32
        ).astype(BF16)
        if c < along_x:
            for k in range(rows):
                grad_send[c, k % pairs * 2 + k // pairs] = part[k * group : (k + 1) * group, :]
            for n, peer in enumerate(x_peers):
                remote(
                    grad_send.at[c, pl.ds(lax.rem(peer[0], pairs) * 2, 2)],
                    by_x.at[c, n],
                    peer,
                    x_out,
                    arrive[c],
                ).start()
        else:
            for k in range(rows):
                grad_send[c, k] = part[k * group : (k + 1) * group, :]
            remote(
                grad_send.at[c, pl.ds((1 - z) * pairs, pairs)],
                by_z.at[c - along_x],
                across,
                z_out,
                arrive[c],
            ).start()
    sent.append((x_out, by_x))
    sent.append((z_out, by_z))

    @pl.when(lead)
    def _():
        await_all(recv_sem, energy_back, energy_all.at[pl.ds(0, far - 1)])
        energy_sum[...] = jnp.sum(energy_all[...], axis=0)
        remote(energy_sum, energy_sum, partner, total_out, total_back).start()
        lead_sent.append((total_out, lambda: energy_sum))

    second = {}
    pair_out, line_out = next(sending), next(sending)
    for c in order:
        second[c] = next(landing)
        if c < along_x:
            await_all(recv_sem, arrive[c], by_x.at[c])
            total = grad_send[c, pl.ds(x * 2, 2)].astype(F32)
            for n in range(pairs - 1):
                total += by_x[c, n].astype(F32)
            pair_send[c] = total.astype(BF16)
            remote(
                pair_send.at[c, 1 - z], pair_recv.at[c], across, pair_out, second[c]
            ).start()
        else:
            n = c - along_x
            await_all(recv_sem, arrive[c], by_z.at[n])
            total = grad_send[c, pl.ds(z * pairs, pairs)].astype(F32) + by_z[n].astype(F32)
            line_send[n] = total.astype(BF16)
            for m, peer in enumerate(x_peers):
                remote(
                    line_send.at[n, lax.rem(peer[0], pairs)],
                    line_recv.at[n, m],
                    peer,
                    line_out,
                    second[c],
                ).start()
    sent.append((pair_out, pair_recv))
    sent.append((line_out, line_recv))

    pl.when(follow)(lambda: await_all(recv_sem, total_back, energy_sum))
    norm_all[i, :, width:] = energy_sum[...]
    pl.when(no_loop)(lambda: await_all(recv_sem, move_back, moved_recv))
    moved = split3(moved_recv[...])
    for c in order:
        span = slice(c * chunk, (c + 1) * chunk)
        before = add3(
            jnp.dot(
                moved,
                one_hot(index_own[steps - 2], c * chunk, chunk).astype(BF16),
                preferred_element_type=F32,
            )
        )
        mask = jnp.sum(one_hot(index_own[steps - 1], c * chunk, chunk), axis=0, keepdims=True)
        if c < along_x:
            await_all(recv_sem, second[c], pair_recv.at[c])
            gradient = pair_send[c, z].astype(F32) + pair_recv[c].astype(F32)
        else:
            n = c - along_x
            await_all(recv_sem, second[c], line_recv.at[n])
            gradient = line_send[n, x].astype(F32) + jnp.sum(line_recv[n].astype(F32), axis=0)
        stepped = before + STEP_SIZE * gradient
        kept_out[:, span] = stepped * mask
        norm_all[i, :, span] = jnp.sum(stepped * stepped, axis=0, keepdims=True)

    out, back = next(sending), next(landing)
    mine = norm_all.at[i]
    for peer in row_peers:
        remote(mine, mine, peer, out, back).start()
    others = norm_all.at[pl.ds(0, rows - 1)]
    sent.append((out, others))
    await_all(recv_sem, back, others)
    sums_out[...] = jnp.sum(norm_all[...], axis=0)

    pl.when(loop)(
        lambda: await_all(send_sem, first_out, first_send.at[pl.ds(0, far - 1)])
    )
    pl.when(no_loop)(lambda: await_all(send_sem, first_out, first_send))
    for out, ref in sent:
        await_all(send_sem, out, ref)

    @pl.when(lead)
    def _():
        for t in range(steps - 1):
            await_all(send_sem, kept_out_sem[t], kept.at[t, pl.ds(0, far - 1)])
        for n in range(CORES):
            pl.when(jnp.logical_not(here[n]))(moves[n].wait_send)
        for out, ref in lead_sent:
            await_all(send_sem, out, ref())

    @pl.when(follow)
    def _():
        for t in range(steps - 1):
            await_all(send_sem, kept_out_sem[t], kept.at[t, pl.ds(0, far)])


def finish(total_count, kept, sums, estimate, norms, energies):
    width = kept.shape[1]
    estimate[...] = kept[...]
    norms[...] = jnp.sqrt(sums[:, :width]).reshape(width)
    for t in range(energies.shape[0]):
        energies[t] = sums[0, width + t] / total_count


def solution(mesh, far=4, high=4, chunk=512, along_x=3):
    rows = mesh.shape["row"]

    def local(matrix, measured, support):
        depth, width = matrix.shape
        signals = measured.shape[0]
        group = signals // rows
        party = CORES * group
        pairs = rows // 2
        steps = support.shape[0]
        turns = steps - 1
        span = min(chunk, width)
        chunks = width // span
        along_z = chunks - along_x
        in_vmem = pl.BlockSpec(memory_space=pltpu.VMEM)
        in_hbm = pl.BlockSpec(memory_space=pltpu.HBM)
        kept, sums = pl.pallas_call(
            functools.partial(kernel, (rows, far, high, along_x)),
            out_shape=(
                jax.ShapeDtypeStruct((group, width), F32),
                jax.ShapeDtypeStruct((1, width + KMAX), F32),
            ),
            in_specs=[in_hbm] * 3,
            out_specs=(in_vmem,) * 2,
            scratch_shapes=[
                pltpu.VMEM(support.shape, jnp.int32),
                pltpu.VMEM(measured.shape, F32),
                pltpu.VMEM((depth, width), BF16),
                pltpu.VMEM((steps, KMAX, 1), jnp.int32),
                pltpu.VMEM((turns, KMAX, 1), jnp.int32),
                pltpu.VMEM((turns, rows, KMAX, depth), BF16),
                pltpu.VMEM((far, party, KMAX), BF16),
                pltpu.VMEM((rows, party, KMAX), BF16),
                pltpu.VMEM((turns, rows, party, KMAX), BF16),
                pltpu.VMEM((turns, rows - 1, party, KMAX), BF16),
                pltpu.VMEM((turns, rows, party, KMAX), BF16),
                pltpu.VMEM((party, KMAX), F32),
                pltpu.VMEM((turns, high, party, depth), BF16),
                pltpu.VMEM((CORES, group, KMAX), F32),
                pltpu.VMEM((group, KMAX), F32),
                pltpu.VMEM((far, party, depth), BF16),
                pltpu.VMEM((far, 1, KMAX), F32),
                pltpu.VMEM((1, KMAX), F32),
                pltpu.VMEM((chunks, rows, group, span), BF16),
                pltpu.VMEM((along_x, pairs - 1, 2, group, span), BF16),
                pltpu.VMEM((along_z, pairs, group, span), BF16),
                pltpu.VMEM((along_x, 2, group, span), BF16),
                pltpu.VMEM((along_x, group, span), BF16),
                pltpu.VMEM((along_z, pairs, group, span), BF16),
                pltpu.VMEM((along_z, pairs - 1, group, span), BF16),
                pltpu.VMEM((rows, 1, width + KMAX), F32),
                pltpu.SemaphoreType.DMA((chunks + 2,)),
                pltpu.SemaphoreType.DMA((22,)),
                pltpu.SemaphoreType.DMA((20 + 2 * chunks,)),
            ],
            compiler_params=pltpu.CompilerParams(
                collective_id=0, has_side_effects=True, vmem_limit_bytes=40 * 2**20
            ),
        )(*(pltpu.with_memory_space_constraint(a, pltpu.HBM) for a in (support, measured, matrix)))
        return pl.pallas_call(
            functools.partial(finish, float(signals * depth * rows)),
            out_shape=(
                jax.ShapeDtypeStruct((group, width), F32),
                jax.ShapeDtypeStruct((width,), F32),
                jax.ShapeDtypeStruct((steps,), F32),
            ),
            in_specs=[in_vmem] * 2,
            out_specs=(in_vmem, in_vmem, pl.BlockSpec(memory_space=pltpu.SMEM)),
            compiler_params=pltpu.CompilerParams(vmem_limit_bytes=4 * 2**20),
        )(kept, sums)

    return jax.shard_map(
        local,
        mesh=mesh,
        in_specs=(P("row", "col"), P(None, "row"), P()),
        out_specs=(P("row", "col"), P("col"), P()),
        check_vma=False,
    )
```

```python
import functools

import jax
import jax.numpy as jnp
from jax import lax
from jax.experimental import pallas as pl
from jax.experimental.pallas import tpu as pltpu
from jax.sharding import PartitionSpec as P

KMAX = 128
STEP_SIZE = 0.25
CORES = 2
LEAD = 1
NEAR = (((1,), (1,)), ((), ()))
F32 = jnp.float32
BF16 = jnp.bfloat16


def iota(shape, dim):
    return lax.broadcasted_iota(jnp.int32, shape, dim)


def window(line, start, width):
    count = line.shape[1]
    below = jnp.sum(jnp.where(line < start, 1.0, 0.0), axis=1, keepdims=True)
    upto = jnp.sum(jnp.where(line < start + width, 1.0, 0.0), axis=1, keepdims=True)
    place = iota((KMAX, count), 1) - iota((KMAX, count), 0)
    local = (line - start).astype(F32)
    found = jnp.sum(
        jnp.where(place == below.astype(jnp.int32), local, 0.0), axis=1, keepdims=True
    )
    there = iota((KMAX, 1), 0).astype(F32) < upto - below
    return jnp.where(there, found, -1.0).astype(jnp.int32)


def one_hot(index, first, width):
    return jnp.where(iota((KMAX, width), 1) + first == index, 1.0, 0.0)


def split3(value):
    high = value.astype(BF16)
    rest = value - high.astype(F32)
    middle = rest.astype(BF16)
    low = (rest - middle.astype(F32)).astype(BF16)
    return jnp.concatenate([high, middle, low], axis=0)


def add3(value):
    third = value.shape[0] // 3
    return value[:third] + value[third : 2 * third] + value[2 * third :]


def kernel(
    shape,
    support_in,
    measured_in,
    matrix,
    kept_out,
    sums_out,
    support,
    measured,
    a_block,
    index_own,
    index_held,
    kept,
    first_send,
    first_recv,
    slope_send,
    slope_recv,
    current_all,
    held,
    seen_all,
    moved_send,
    moved_recv,
    residual_all,
    energy_all,
    energy_sum,
    near_x,
    near_z,
    near_by_x,
    near_by_z,
    rest_x,
    rest_z,
    rest_by_x,
    rest_by_z,
    pair_send,
    pair_recv,
    line_send,
    line_recv,
    norm_all,
    load_sem,
    send_sem,
    recv_sem,
):
    rows, far, high, along_x = shape
    pairs = rows // 2
    depth, width = matrix.shape
    group = measured.shape[0] // rows
    part = group // far
    party = rows * part
    steps = support.shape[0]
    chunk = near_x.shape[3]
    chunks = width // chunk
    i = lax.axis_index("row")
    col = lax.axis_index("col")
    x = lax.rem(i, pairs)
    z = i // pairs
    core = lax.rem(col, CORES)
    h = lax.rem(col // CORES, high)
    y = col // (CORES * high)
    q = y * CORES + core
    lead = core == LEAD
    follow = core != LEAD
    sending = iter(range(send_sem.shape[0]))
    landing = iter(range(recv_sem.shape[0]))
    sent = []
    lead_sent = []

    def at(yy, hh, cc):
        return (yy * high + hh) * CORES + cc

    def member(k):
        return at(k // CORES, h, lax.rem(k, CORES))

    def far_first(count):
        return sorted(range(1, count), key=lambda d: -min(d, count - d))

    def remote(src, dst, where, out, back):
        return pltpu.make_async_remote_copy(
            src_ref=src,
            dst_ref=dst,
            send_sem=send_sem.at[out],
            recv_sem=recv_sem.at[back],
            device_id=where,
            device_id_type=pl.DeviceIdType.MESH,
        )

    def await_all(sems, slot, ref):
        pltpu.make_async_copy(ref, ref, sems.at[slot]).wait()

    x_shift = far_first(pairs)
    offsets = [(1, d) for d in x_shift] + [(0, d) for d in x_shift] + [(1, 0)]
    row_peers = [
        (lax.rem(z + dz, 2) * pairs + lax.rem(x + dx, pairs), col) for dz, dx in offsets
    ]
    x_peers = [(z * pairs + lax.rem(x + d, pairs), col) for d in x_shift]
    across = ((1 - z) * pairs + x, col)
    y_shift = far_first(far)
    y_near = [lax.rem(y + d, far) for d in y_shift]
    y_from = [lax.rem(y - d + far, far) for d in y_shift]
    y_leads = [(i, at(yy, h, LEAD)) for yy in y_near]
    h_peers = [(i, at(y, lax.rem(h + d, high), core)) for d in far_first(high)]
    partner = (i, at(y, h, 1 - core))
    def rows_of(k, yy):
        return pl.ds(pl.multiple_of(k * group + yy * part, part), part)

    support_load = pltpu.make_async_copy(support_in, support, load_sem.at[chunks])
    support_load.start()
    loads = [
        pltpu.make_async_copy(
            matrix.at[:, pl.ds(c * chunk, chunk)],
            a_block.at[:, pl.ds(c * chunk, chunk)],
            load_sem.at[c],
        )
        for c in range(chunks)
    ]
    for load in loads:
        load.start()
    measured_load = pltpu.make_async_copy(measured_in, measured, load_sem.at[chunks + 1])
    measured_load.start()
    barrier = pltpu.get_barrier_semaphore()

    def greet(peer):
        pl.semaphore_signal(
            barrier, inc=1, device_id=peer, device_id_type=pl.DeviceIdType.MESH
        )

    on_diagonal = i == q
    loop = jnp.logical_and(on_diagonal, lead)
    no_loop = jnp.logical_not(loop)
    for k in range(far):
        pl.when(jnp.logical_or(no_loop, y != k))(lambda k=k: greet((q, at(k, h, LEAD))))
    for peer in row_peers + [partner]:
        greet(peer)

    @pl.when(lead)
    def _():
        for k in range(rows):
            pl.when(jnp.logical_or(jnp.logical_not(on_diagonal), i != k))(
                lambda k=k: greet((k, member(i)))
            )
        for yy in y_near:
            for cc in range(CORES):
                greet((i, at(yy, h, cc)))
        for peer in h_peers:
            greet(peer)

    greetings = (
        len(row_peers) + 1 + len(y_leads) + far
        + jnp.where(lead, len(h_peers) + rows, 0)
        - jnp.where(loop, 2, 0)
    )

    support_load.wait()

    def find_own(t):
        index_own[t] = window(support[t : t + 1, :], col * width, width)

    def pick(first, last, loaded):
        total = jnp.zeros(((last - first) * KMAX, depth), F32)
        for c in range(chunks):
            if not loaded:
                loads[c].wait()
            hot = jnp.concatenate(
                [one_hot(index_own[t], c * chunk, chunk).astype(BF16) for t in range(first, last)],
                axis=0,
            )
            total += lax.dot_general(
                hot, a_block[:, c * chunk : (c + 1) * chunk], NEAR, preferred_element_type=F32
            )
        for t in range(first, last):
            kept[t, q] = total[(t - first) * KMAX : (t - first + 1) * KMAX, :].astype(BF16)

    find_own(0)
    pick(0, 1, False)
    measured_load.wait()

    first = lax.dot_general(
        measured[...].astype(BF16), kept[0, q], NEAR, preferred_element_type=F32
    )
    for n in range(far):
        first_send[n] = jnp.concatenate(
            [first[k * group + n * part :][:part] for k in range(rows)], axis=0
        ).astype(BF16)

    pl.semaphore_wait(barrier, greetings)

    first_out, first_back = next(sending), next(landing)
    for k in range(far):
        copy = remote(
            first_send.at[k], first_recv.at[i], (q, at(k, h, LEAD)), first_out, first_back
        )
        other = jnp.logical_or(no_loop, y != k)
        pl.when(other)(copy.start)

        @pl.when(jnp.logical_not(other))
        def _():
            first_recv[i] = first_send[k]

    kept_out_sem = [next(sending) for _ in range(steps - 1)]
    kept_back = [next(landing) for _ in range(steps - 1)]

    def spread(t):
        own = kept.at[t, q]
        for peer in y_leads:
            remote(own, own, peer, kept_out_sem[t], kept_back[t]).start()
        pl.when(follow)(remote(own, own, partner, kept_out_sem[t], kept_back[t]).start)

    spread(0)
    for t in range(1, steps - 1):
        find_own(t)
    pick(1, steps - 1, True)
    for t in range(1, steps - 1):
        spread(t)
    find_own(steps - 1)

    def carried(t, value):
        diagonal = iota((KMAX, KMAX), 0) == iota((KMAX, KMAX), 1)
        after = jnp.sum(
            jnp.where(diagonal, index_held[t + 1].astype(F32), 0.0), axis=0, keepdims=True
        ).astype(jnp.int32)
        before = index_held[t]
        same = jnp.where(jnp.logical_and(before == after, before >= 0), 1.0, 0.0).astype(BF16)
        return add3(jnp.dot(split3(value), same, preferred_element_type=F32))

    move_out, move_back = next(sending), next(landing)
    energy_out, energy_back, total_out, total_back = (
        next(sending), next(landing), next(sending), next(landing)
    )
    r_out, r_back = next(sending), [next(landing) for _ in y_leads]
    pass_out, own_back, pass_back = next(sending), next(landing), next(landing)
    moves = [
        remote(moved_send.at[k], moved_recv.at[y], (k, member(i)), move_out, move_back)
        for k in range(rows)
    ]
    here = [jnp.logical_and(on_diagonal, i == k) for k in range(rows)]

    @pl.when(lead)
    def _():
        for t in range(steps - 1):
            index_held[t] = window(support[t : t + 1, :], member(i) * width, width)
        pl.when(on_diagonal)(
            lambda: await_all(recv_sem, first_back, first_recv.at[pl.ds(0, rows - 1)])
        )
        pl.when(jnp.logical_not(on_diagonal))(lambda: await_all(recv_sem, first_back, first_recv))
        current = STEP_SIZE * jnp.sum(first_recv[...].astype(F32), axis=0)

        own_measured = jnp.concatenate(
            [measured[rows_of(k, y), :] for k in range(rows)], axis=0
        )
        energy = [jnp.sum(own_measured * own_measured)]
        for t in range(steps - 1):
            if t > 0:
                await_all(recv_sem, kept_back[t], kept.at[t, pl.ds(0, rows - 1)])
                slope = lax.dot_general(
                    residual.astype(BF16),
                    kept[t].reshape(rows * KMAX, depth),
                    NEAR,
                    preferred_element_type=F32,
                ).astype(BF16)
                for k in range(rows):
                    slope_send[t - 1, k] = slope[:, k * KMAX : (k + 1) * KMAX]
                out, back = next(sending), next(landing)
                for n, peer in enumerate(row_peers):
                    remote(
                        slope_send.at[t - 1, peer[0]], slope_recv.at[t - 1, n], peer, out, back
                    ).start()
                lead_sent.append((out, lambda t=t: slope_recv.at[t - 1]))
                carry = carried(t - 1, held[...])
                await_all(recv_sem, back, slope_recv.at[t - 1])
                gathered = slope_send[t - 1, i].astype(F32) + jnp.sum(
                    slope_recv[t - 1].astype(F32), axis=0
                )
                current = carry + STEP_SIZE * gathered
            held[...] = current
            current_all[t, i] = current.astype(BF16)
            out, back = next(sending), next(landing)
            mine = current_all.at[t, i]
            for peer in row_peers:
                remote(mine, mine, peer, out, back).start()
            others = current_all.at[t, pl.ds(0, rows - 1)]
            lead_sent.append((out, lambda t=t: current_all.at[t, pl.ds(0, rows - 1)]))
            if t == steps - 2:
                for k in range(rows):
                    moved_send[k] = current[k * part : (k + 1) * part, :]
                    pl.when(jnp.logical_not(here[k]))(moves[k].start)

                    @pl.when(here[k])
                    def _():
                        moved_recv[y] = moved_send[k]

            if t == 0:
                await_all(recv_sem, kept_back[t], kept.at[t, pl.ds(0, rows - 1)])
            await_all(recv_sem, back, others)
            signals = jnp.concatenate([current_all[t, k] for k in range(rows)], axis=1)
            seen_all[t, h] = jnp.dot(
                signals, kept[t].reshape(rows * KMAX, depth), preferred_element_type=F32
            ).astype(BF16)
            out, back = next(sending), next(landing)
            mine = seen_all.at[t, h]
            for peer in h_peers:
                remote(mine, mine, peer, out, back).start()
            others = seen_all.at[t, pl.ds(0, high - 1)]
            lead_sent.append((out, lambda t=t: seen_all.at[t, pl.ds(0, high - 1)]))
            await_all(recv_sem, back, others)
            residual = own_measured - jnp.sum(seen_all[t].astype(F32), axis=0)
            energy.append(jnp.sum(residual * residual))

        residual_all[y] = residual.astype(BF16)
        own = residual_all.at[y]
        for n, peer in enumerate(y_leads):
            remote(own, own, peer, r_out, r_back[n]).start()
        remote(own, own, partner, pass_out, own_back).start()
        lanes = iota((1, KMAX), 1)
        values = jnp.zeros((1, KMAX), F32)
        for t in range(steps):
            values = jnp.where(lanes == t, energy[t], values)
        energy_all[y] = values
        mine = energy_all.at[y]
        for peer in y_leads:
            remote(mine, mine, peer, energy_out, energy_back).start()
        lead_sent.append((r_out, lambda: residual_all.at[pl.ds(0, far - 1)]))
        lead_sent.append((pass_out, lambda: residual_all))
        lead_sent.append((energy_out, lambda: energy_all.at[pl.ds(0, far - 1)]))

    pl.when(follow)(lambda: await_all(recv_sem, own_back, residual_all.at[0]))

    z_out, x_out, near_z_out, near_x_out = (next(sending) for _ in range(4))
    near_back = [next(landing) for _ in range(chunks)]
    rest_back = [next(landing) for _ in range(chunks)]
    first_by_x = list(range(along_x))
    across_first = list(range(along_x, chunks))
    order = []
    for n in range(max(len(first_by_x), len(across_first))):
        order += across_first[n : n + 1] + first_by_x[n : n + 1]

    def send_dense(lhs, to_x, to_z, from_x, from_z, out_x, out_z, back):
        count = lhs.shape[0] // party

        def tile(product, k):
            return [product[n * party + k * part :][:part] for n in range(count)]

        for c in order:
            product = jnp.dot(
                lhs, a_block[:, c * chunk : (c + 1) * chunk], preferred_element_type=F32
            )
            if c < along_x:
                for k in range(pairs):
                    to_x[c, k] = jnp.concatenate(
                        tile(product, k) + tile(product, pairs + k), axis=0
                    ).astype(BF16)
                for n, peer in enumerate(x_peers):
                    remote(
                        to_x.at[c, lax.rem(peer[0], pairs)], from_x.at[c, n], peer, out_x, back[c]
                    ).start()
            else:
                n = c - along_x
                for k in range(2):
                    to_z[n, k] = jnp.concatenate(
                        sum([tile(product, k * pairs + m) for m in range(pairs)], []), axis=0
                    ).astype(BF16)
                remote(to_z.at[n, 1 - z], from_z.at[n], across, out_z, back[c]).start()
        sent.append((out_x, from_x))
        sent.append((out_z, from_z))

    send_dense(
        residual_all[y], near_x, near_z, near_by_x, near_by_z, near_x_out, near_z_out, near_back
    )

    @pl.when(lead)
    def _():
        for n, yy in enumerate(y_from):
            slot = residual_all.at[yy]
            await_all(recv_sem, r_back[n], slot)
            remote(slot, slot, partner, pass_out, pass_back).start()

    pl.when(follow)(lambda: await_all(recv_sem, pass_back, residual_all.at[pl.ds(0, far - 1)]))
    send_dense(
        jnp.concatenate([residual_all[yy] for yy in y_from], axis=0),
        rest_x, rest_z, rest_by_x, rest_by_z, x_out, z_out, rest_back,
    )

    @pl.when(lead)
    def _():
        await_all(recv_sem, energy_back, energy_all.at[pl.ds(0, far - 1)])
        energy_sum[...] = jnp.sum(energy_all[...], axis=0)
        remote(energy_sum, energy_sum, partner, total_out, total_back).start()
        lead_sent.append((total_out, lambda: energy_sum))

    rest = part * (far - 1)
    second = {}
    pair_out, line_out = next(sending), next(sending)
    for c in order:
        second[c] = next(landing)
        if c < along_x:
            await_all(recv_sem, near_back[c], near_by_x.at[c])
            near = near_x[c, x].astype(F32) + jnp.sum(near_by_x[c].astype(F32), axis=0)
            await_all(recv_sem, rest_back[c], rest_by_x.at[c])
            total = rest_x[c, x].astype(F32) + jnp.sum(rest_by_x[c].astype(F32), axis=0)
            for k in range(2):
                pair_send[c, k] = jnp.concatenate(
                    [near[k * part :][:part], total[k * rest :][:rest]], axis=0
                ).astype(BF16)
            remote(
                pair_send.at[c, 1 - z], pair_recv.at[c], across, pair_out, second[c]
            ).start()
        else:
            n = c - along_x
            await_all(recv_sem, near_back[c], near_by_z.at[n])
            near = near_z[n, z].astype(F32) + near_by_z[n].astype(F32)
            await_all(recv_sem, rest_back[c], rest_by_z.at[n])
            total = rest_z[n, z].astype(F32) + rest_by_z[n].astype(F32)
            for k in range(pairs):
                line_send[n, k] = jnp.concatenate(
                    [near[k * part :][:part], total[k * rest :][:rest]], axis=0
                ).astype(BF16)
            for m, peer in enumerate(x_peers):
                remote(
                    line_send.at[n, lax.rem(peer[0], pairs)],
                    line_recv.at[n, m],
                    peer,
                    line_out,
                    second[c],
                ).start()
    sent.append((pair_out, pair_recv))
    sent.append((line_out, line_recv))

    pl.when(follow)(lambda: await_all(recv_sem, total_back, energy_sum))
    norm_all[i, :, width:] = energy_sum[...]
    pl.when(loop)(lambda: await_all(recv_sem, move_back, moved_recv.at[pl.ds(0, far - 1)]))
    pl.when(no_loop)(lambda: await_all(recv_sem, move_back, moved_recv))
    y_order = [y] + y_from
    moved = split3(jnp.concatenate([moved_recv[yy] for yy in y_order], axis=0))
    for c in order:
        span = slice(c * chunk, (c + 1) * chunk)
        before = add3(
            jnp.dot(
                moved,
                one_hot(index_own[steps - 2], c * chunk, chunk).astype(BF16),
                preferred_element_type=F32,
            )
        )
        mask = jnp.sum(one_hot(index_own[steps - 1], c * chunk, chunk), axis=0, keepdims=True)
        if c < along_x:
            await_all(recv_sem, second[c], pair_recv.at[c])
            gradient = pair_send[c, z].astype(F32) + pair_recv[c].astype(F32)
        else:
            n = c - along_x
            await_all(recv_sem, second[c], line_recv.at[n])
            gradient = line_send[n, x].astype(F32) + jnp.sum(line_recv[n].astype(F32), axis=0)
        stepped = before + STEP_SIZE * gradient
        settled = stepped * mask
        for n, yy in enumerate(y_order):
            kept_out[rows_of(0, yy), span] = settled[n * part : (n + 1) * part]
        norm_all[i, :, span] = jnp.sum(stepped * stepped, axis=0, keepdims=True)

    out, back = next(sending), next(landing)
    mine = norm_all.at[i]
    for peer in row_peers:
        remote(mine, mine, peer, out, back).start()
    others = norm_all.at[pl.ds(0, rows - 1)]
    sent.append((out, others))
    await_all(recv_sem, back, others)
    sums_out[...] = jnp.sum(norm_all[...], axis=0)

    pl.when(loop)(
        lambda: await_all(send_sem, first_out, first_send.at[pl.ds(0, far - 1)])
    )
    pl.when(no_loop)(lambda: await_all(send_sem, first_out, first_send))
    for out, ref in sent:
        await_all(send_sem, out, ref)

    @pl.when(lead)
    def _():
        for t in range(steps - 1):
            await_all(send_sem, kept_out_sem[t], kept.at[t, pl.ds(0, far - 1)])
        for k in range(rows):
            pl.when(jnp.logical_not(here[k]))(moves[k].wait_send)
        for out, ref in lead_sent:
            await_all(send_sem, out, ref())

    @pl.when(follow)
    def _():
        for t in range(steps - 1):
            await_all(send_sem, kept_out_sem[t], kept.at[t, pl.ds(0, far)])


def finish(total_count, kept, sums, estimate, norms, energies):
    width = kept.shape[1]
    estimate[...] = kept[...]
    norms[...] = jnp.sqrt(sums[:, :width]).reshape(width)
    for t in range(energies.shape[0]):
        energies[t] = sums[0, width + t] / total_count


def solution(mesh, far=4, high=4, chunk=512, along_x=3):
    rows = mesh.shape["row"]

    def local(matrix, measured, support):
        depth, width = matrix.shape
        signals = measured.shape[0]
        group = signals // rows
        part = group // far
        party = rows * part
        rest = part * (far - 1)
        pairs = rows // 2
        steps = support.shape[0]
        turns = steps - 1
        span = min(chunk, width)
        chunks = width // span
        along_z = chunks - along_x
        in_vmem = pl.BlockSpec(memory_space=pltpu.VMEM)
        in_hbm = pl.BlockSpec(memory_space=pltpu.HBM)
        kept, sums = pl.pallas_call(
            functools.partial(kernel, (rows, far, high, along_x)),
            out_shape=(
                jax.ShapeDtypeStruct((group, width), F32),
                jax.ShapeDtypeStruct((1, width + KMAX), F32),
            ),
            in_specs=[in_hbm] * 3,
            out_specs=(in_vmem,) * 2,
            scratch_shapes=[
                pltpu.VMEM(support.shape, jnp.int32),
                pltpu.VMEM(measured.shape, F32),
                pltpu.VMEM((depth, width), BF16),
                pltpu.VMEM((steps, KMAX, 1), jnp.int32),
                pltpu.VMEM((turns, KMAX, 1), jnp.int32),
                pltpu.VMEM((turns, rows, KMAX, depth), BF16),
                pltpu.VMEM((far, party, KMAX), BF16),
                pltpu.VMEM((rows, party, KMAX), BF16),
                pltpu.VMEM((turns, rows, party, KMAX), BF16),
                pltpu.VMEM((turns, rows - 1, party, KMAX), BF16),
                pltpu.VMEM((turns, rows, party, KMAX), BF16),
                pltpu.VMEM((party, KMAX), F32),
                pltpu.VMEM((turns, high, party, depth), BF16),
                pltpu.VMEM((rows, part, KMAX), F32),
                pltpu.VMEM((far, part, KMAX), F32),
                pltpu.VMEM((far, party, depth), BF16),
                pltpu.VMEM((far, 1, KMAX), F32),
                pltpu.VMEM((1, KMAX), F32),
                pltpu.VMEM((along_x, pairs, 2 * part, span), BF16),
                pltpu.VMEM((along_z, 2, pairs * part, span), BF16),
                pltpu.VMEM((along_x, pairs - 1, 2 * part, span), BF16),
                pltpu.VMEM((along_z, pairs * part, span), BF16),
                pltpu.VMEM((along_x, pairs, 2 * rest, span), BF16),
                pltpu.VMEM((along_z, 2, pairs * rest, span), BF16),
                pltpu.VMEM((along_x, pairs - 1, 2 * rest, span), BF16),
                pltpu.VMEM((along_z, pairs * rest, span), BF16),
                pltpu.VMEM((along_x, 2, group, span), BF16),
                pltpu.VMEM((along_x, group, span), BF16),
                pltpu.VMEM((along_z, pairs, group, span), BF16),
                pltpu.VMEM((along_z, pairs - 1, group, span), BF16),
                pltpu.VMEM((rows, 1, width + KMAX), F32),
                pltpu.SemaphoreType.DMA((chunks + 2,)),
                pltpu.SemaphoreType.DMA((24,)),
                pltpu.SemaphoreType.DMA((21 + 3 * chunks,)),
            ],
            compiler_params=pltpu.CompilerParams(
                collective_id=0, has_side_effects=True, vmem_limit_bytes=40 * 2**20
            ),
        )(*(pltpu.with_memory_space_constraint(a, pltpu.HBM) for a in (support, measured, matrix)))
        return pl.pallas_call(
            functools.partial(finish, float(signals * depth * rows)),
            out_shape=(
                jax.ShapeDtypeStruct((group, width), F32),
                jax.ShapeDtypeStruct((width,), F32),
                jax.ShapeDtypeStruct((steps,), F32),
            ),
            in_specs=[in_vmem] * 2,
            out_specs=(in_vmem, in_vmem, pl.BlockSpec(memory_space=pltpu.SMEM)),
            compiler_params=pltpu.CompilerParams(vmem_limit_bytes=4 * 2**20),
        )(kept, sums)

    return jax.shard_map(
        local,
        mesh=mesh,
        in_specs=(P("row", "col"), P(None, "row"), P()),
        out_specs=(P("row", "col"), P("col"), P()),
        check_vma=False,
    )
```

```python
import functools

import jax
import jax.numpy as jnp
from jax import lax
from jax.experimental import pallas as pl
from jax.experimental.pallas import tpu as pltpu
from jax.sharding import PartitionSpec as P

KMAX = 128
STEP_SIZE = 0.25
CORES = 2
LEAD = 1
NEAR = (((1,), (1,)), ((), ()))
F32 = jnp.float32
BF16 = jnp.bfloat16


def iota(shape, dim):
    return lax.broadcasted_iota(jnp.int32, shape, dim)


def window(line, start, width):
    count = line.shape[1]
    below = jnp.sum(jnp.where(line < start, 1.0, 0.0), axis=1, keepdims=True)
    upto = jnp.sum(jnp.where(line < start + width, 1.0, 0.0), axis=1, keepdims=True)
    place = iota((KMAX, count), 1) - iota((KMAX, count), 0)
    local = (line - start).astype(F32)
    found = jnp.sum(
        jnp.where(place == below.astype(jnp.int32), local, 0.0), axis=1, keepdims=True
    )
    there = iota((KMAX, 1), 0).astype(F32) < upto - below
    return jnp.where(there, found, -1.0).astype(jnp.int32)


def one_hot(index, first, width):
    return jnp.where(iota((KMAX, width), 1) + first == index, 1.0, 0.0)


def split3(value):
    high = value.astype(BF16)
    rest = value - high.astype(F32)
    middle = rest.astype(BF16)
    low = (rest - middle.astype(F32)).astype(BF16)
    return jnp.concatenate([high, middle, low], axis=0)


def add3(value):
    third = value.shape[0] // 3
    return value[:third] + value[third : 2 * third] + value[2 * third :]


def kernel(
    shape,
    support_in,
    measured_in,
    matrix,
    kept_out,
    sums_out,
    support,
    measured,
    a_block,
    index_own,
    index_held,
    kept,
    first_send,
    first_recv,
    slope_send,
    slope_recv,
    current_all,
    held,
    seen_all,
    moved_send,
    moved_recv,
    residual_all,
    energy_all,
    energy_sum,
    near_x,
    near_z,
    near_by_x,
    near_by_z,
    rest_x,
    rest_z,
    rest_by_x,
    rest_by_z,
    pair_send,
    pair_recv,
    line_send,
    line_recv,
    norm_all,
    load_sem,
    send_sem,
    recv_sem,
):
    rows, far, high, along_x = shape
    pairs = rows // 2
    depth, width = matrix.shape
    group = measured.shape[0] // rows
    part = group // far
    party = rows * part
    steps = support.shape[0]
    chunk = near_x.shape[3]
    chunks = width // chunk
    i = lax.axis_index("row")
    col = lax.axis_index("col")
    x = lax.rem(i, pairs)
    z = i // pairs
    core = lax.rem(col, CORES)
    h = lax.rem(col // CORES, high)
    y = col // (CORES * high)
    q = y * CORES + core
    lead = core == LEAD
    follow = core != LEAD
    sending = iter(range(send_sem.shape[0]))
    landing = iter(range(recv_sem.shape[0]))
    sent = []
    lead_sent = []

    def at(yy, hh, cc):
        return (yy * high + hh) * CORES + cc

    def member(k):
        return at(k // CORES, h, lax.rem(k, CORES))

    def far_first(count):
        return sorted(range(1, count), key=lambda d: -min(d, count - d))

    def remote(src, dst, where, out, back):
        return pltpu.make_async_remote_copy(
            src_ref=src,
            dst_ref=dst,
            send_sem=send_sem.at[out],
            recv_sem=recv_sem.at[back],
            device_id=where,
            device_id_type=pl.DeviceIdType.MESH,
        )

    def await_all(sems, slot, ref):
        pltpu.make_async_copy(ref, ref, sems.at[slot]).wait()

    x_shift = far_first(pairs)
    offsets = [(1, d) for d in x_shift] + [(0, d) for d in x_shift] + [(1, 0)]
    row_peers = [
        (lax.rem(z + dz, 2) * pairs + lax.rem(x + dx, pairs), col) for dz, dx in offsets
    ]
    x_peers = [(z * pairs + lax.rem(x + d, pairs), col) for d in x_shift]
    across = ((1 - z) * pairs + x, col)
    y_shift = far_first(far)
    y_near = [lax.rem(y + d, far) for d in y_shift]
    y_from = [lax.rem(y - d + far, far) for d in y_shift]
    y_leads = [(i, at(yy, h, LEAD)) for yy in y_near]
    h_peers = [(i, at(y, lax.rem(h + d, high), core)) for d in far_first(high)]
    partner = (i, at(y, h, 1 - core))
    def rows_of(k, yy):
        return pl.ds(pl.multiple_of(k * group + yy * part, part), part)

    support_load = pltpu.make_async_copy(support_in, support, load_sem.at[chunks])
    support_load.start()
    loads = [
        pltpu.make_async_copy(
            matrix.at[:, pl.ds(c * chunk, chunk)],
            a_block.at[:, pl.ds(c * chunk, chunk)],
            load_sem.at[c],
        )
        for c in range(chunks)
    ]
    for load in loads:
        load.start()
    measured_load = pltpu.make_async_copy(measured_in, measured, load_sem.at[chunks + 1])
    measured_load.start()
    barrier = pltpu.get_barrier_semaphore()

    def greet(peer):
        pl.semaphore_signal(
            barrier, inc=1, device_id=peer, device_id_type=pl.DeviceIdType.MESH
        )

    on_diagonal = i == q
    loop = jnp.logical_and(on_diagonal, lead)
    no_loop = jnp.logical_not(loop)

    @pl.when(lead)
    def _():
        for k in range(rows):
            pl.when(jnp.logical_or(jnp.logical_not(on_diagonal), i != k))(
                lambda k=k: greet((k, member(i)))
            )
        for peer in h_peers:
            greet(peer)

    for k in range(far):
        pl.when(jnp.logical_or(no_loop, y != k))(lambda k=k: greet((q, at(k, h, LEAD))))
    for peer in row_peers + [partner]:
        greet(peer)

    @pl.when(lead)
    def _():
        for yy in y_near:
            for cc in range(CORES):
                greet((i, at(yy, h, cc)))

    greetings = (
        len(row_peers) + 1 + len(y_leads) + far
        + jnp.where(lead, len(h_peers) + rows, 0)
        - jnp.where(loop, 2, 0)
    )

    support_load.wait()

    def find_own(t):
        index_own[t] = window(support[t : t + 1, :], col * width, width)

    def pick(first, last, loaded):
        total = jnp.zeros(((last - first) * KMAX, depth), F32)
        for c in range(chunks):
            if not loaded:
                loads[c].wait()
            hot = jnp.concatenate(
                [one_hot(index_own[t], c * chunk, chunk).astype(BF16) for t in range(first, last)],
                axis=0,
            )
            total += lax.dot_general(
                hot, a_block[:, c * chunk : (c + 1) * chunk], NEAR, preferred_element_type=F32
            )
        for t in range(first, last):
            kept[t, q] = total[(t - first) * KMAX : (t - first + 1) * KMAX, :].astype(BF16)

    find_own(0)
    pick(0, 1, False)
    measured_load.wait()

    first = lax.dot_general(
        measured[...].astype(BF16), kept[0, q], NEAR, preferred_element_type=F32
    )
    for n in range(far):
        first_send[n] = jnp.concatenate(
            [first[k * group + n * part :][:part] for k in range(rows)], axis=0
        ).astype(BF16)

    pl.semaphore_wait(barrier, greetings)

    first_out, first_back = next(sending), next(landing)
    for k in range(far):
        copy = remote(
            first_send.at[k], first_recv.at[i], (q, at(k, h, LEAD)), first_out, first_back
        )
        other = jnp.logical_or(no_loop, y != k)
        pl.when(other)(copy.start)

        @pl.when(jnp.logical_not(other))
        def _():
            first_recv[i] = first_send[k]

    kept_out_sem = [next(sending) for _ in range(steps - 1)]
    kept_back = [next(landing) for _ in range(steps - 1)]

    def spread(t):
        own = kept.at[t, q]
        for peer in y_leads:
            remote(own, own, peer, kept_out_sem[t], kept_back[t]).start()
        pl.when(follow)(lambda: remote(own, own, partner, kept_out_sem[t], kept_back[t]).start())

    spread(0)
    for t in range(1, steps - 1):
        find_own(t)
    pick(1, steps - 1, True)
    find_own(steps - 1)

    @pl.when(follow)
    def _():
        for t in range(1, steps - 1):
            await_all(send_sem, kept_out_sem[t - 1], kept.at[t - 1, pl.ds(0, far)])
            spread(t)


    def carried(t, value):
        diagonal = iota((KMAX, KMAX), 0) == iota((KMAX, KMAX), 1)
        after = jnp.sum(
            jnp.where(diagonal, index_held[t + 1].astype(F32), 0.0), axis=0, keepdims=True
        ).astype(jnp.int32)
        before = index_held[t]
        same = jnp.where(jnp.logical_and(before == after, before >= 0), 1.0, 0.0).astype(BF16)
        return add3(jnp.dot(split3(value), same, preferred_element_type=F32))

    move_out, move_back = next(sending), next(landing)
    energy_out, energy_back, total_out, total_back = (
        next(sending), next(landing), next(sending), next(landing)
    )
    r_out, r_back = next(sending), [next(landing) for _ in y_leads]
    pass_out, own_back, pass_back = next(sending), next(landing), next(landing)
    moves = [
        remote(moved_send.at[k], moved_recv.at[y], (k, member(i)), move_out, move_back)
        for k in range(rows)
    ]
    here = [jnp.logical_and(on_diagonal, i == k) for k in range(rows)]

    @pl.when(lead)
    def _():
        for t in range(steps - 1):
            index_held[t] = window(support[t : t + 1, :], member(i) * width, width)
        pl.when(on_diagonal)(
            lambda: await_all(recv_sem, first_back, first_recv.at[pl.ds(0, rows - 1)])
        )
        pl.when(jnp.logical_not(on_diagonal))(lambda: await_all(recv_sem, first_back, first_recv))
        current = STEP_SIZE * jnp.sum(first_recv[...].astype(F32), axis=0)

        own_measured = jnp.concatenate(
            [measured[rows_of(k, y), :] for k in range(rows)], axis=0
        )
        energy = [jnp.sum(own_measured * own_measured)]
        for t in range(steps - 1):
            if t > 0:
                await_all(recv_sem, kept_back[t], kept.at[t, pl.ds(0, rows - 1)])
                slope = lax.dot_general(
                    residual.astype(BF16),
                    kept[t].reshape(rows * KMAX, depth),
                    NEAR,
                    preferred_element_type=F32,
                ).astype(BF16)
                for k in range(rows):
                    slope_send[t - 1, k] = slope[:, k * KMAX : (k + 1) * KMAX]
                out, back = next(sending), next(landing)
                for n, peer in enumerate(row_peers):
                    remote(
                        slope_send.at[t - 1, peer[0]], slope_recv.at[t - 1, n], peer, out, back
                    ).start()
                lead_sent.append((out, lambda t=t: slope_recv.at[t - 1]))
                carry = carried(t - 1, held[...])
                await_all(recv_sem, back, slope_recv.at[t - 1])
                gathered = slope_send[t - 1, i].astype(F32) + jnp.sum(
                    slope_recv[t - 1].astype(F32), axis=0
                )
                current = carry + STEP_SIZE * gathered
            held[...] = current
            current_all[t, i] = current.astype(BF16)
            out, back = next(sending), next(landing)
            mine = current_all.at[t, i]
            for peer in row_peers:
                remote(mine, mine, peer, out, back).start()
            others = current_all.at[t, pl.ds(0, rows - 1)]
            lead_sent.append((out, lambda t=t: current_all.at[t, pl.ds(0, rows - 1)]))
            if t == steps - 2:
                for k in range(rows):
                    moved_send[k] = current[k * part : (k + 1) * part, :]
                    pl.when(jnp.logical_not(here[k]))(moves[k].start)

                    @pl.when(here[k])
                    def _():
                        moved_recv[y] = moved_send[k]

            if t < steps - 2:
                spread(t + 1)
            if t == 0:
                await_all(recv_sem, kept_back[t], kept.at[t, pl.ds(0, rows - 1)])
            await_all(recv_sem, back, others)
            signals = jnp.concatenate([current_all[t, k] for k in range(rows)], axis=1)
            seen_all[t, h] = jnp.dot(
                signals, kept[t].reshape(rows * KMAX, depth), preferred_element_type=F32
            ).astype(BF16)
            out, back = next(sending), next(landing)
            mine = seen_all.at[t, h]
            for peer in h_peers:
                remote(mine, mine, peer, out, back).start()
            others = seen_all.at[t, pl.ds(0, high - 1)]
            lead_sent.append((out, lambda t=t: seen_all.at[t, pl.ds(0, high - 1)]))
            await_all(recv_sem, back, others)
            residual = own_measured - jnp.sum(seen_all[t].astype(F32), axis=0)
            energy.append(jnp.sum(residual * residual))

        residual_all[y] = residual.astype(BF16)
        own = residual_all.at[y]
        for n, peer in enumerate(y_leads):
            remote(own, own, peer, r_out, r_back[n]).start()
        remote(own, own, partner, pass_out, own_back).start()
        lanes = iota((1, KMAX), 1)
        values = jnp.zeros((1, KMAX), F32)
        for t in range(steps):
            values = jnp.where(lanes == t, energy[t], values)
        energy_all[y] = values
        mine = energy_all.at[y]
        for peer in y_leads:
            remote(mine, mine, peer, energy_out, energy_back).start()
        lead_sent.append((r_out, lambda: residual_all.at[pl.ds(0, far - 1)]))
        lead_sent.append((pass_out, lambda: residual_all))
        lead_sent.append((energy_out, lambda: energy_all.at[pl.ds(0, far - 1)]))

    pl.when(follow)(lambda: await_all(recv_sem, own_back, residual_all.at[0]))

    z_out, x_out, near_z_out, near_x_out = (next(sending) for _ in range(4))
    near_back = [next(landing) for _ in range(chunks)]
    rest_back = [next(landing) for _ in range(chunks)]
    first_by_x = list(range(along_x))
    across_first = list(range(along_x, chunks))
    order = []
    for n in range(max(len(first_by_x), len(across_first))):
        order += first_by_x[n : n + 1] + across_first[n : n + 1]

    def send_dense(lhs, to_x, to_z, from_x, from_z, out_x, out_z, back):
        count = lhs.shape[0] // party

        def launch(c):
            if c < along_x:
                for n, peer in enumerate(x_peers):
                    remote(
                        to_x.at[c, lax.rem(peer[0], pairs)], from_x.at[c, n], peer, out_x, back[c]
                    ).start()
            else:
                n = c - along_x
                remote(to_z.at[n, 1 - z], from_z.at[n], across, out_z, back[c]).start()

        def tile(product, k):
            return [product[n * party + k * part :][:part] for n in range(count)]

        for c in order:
            product = jnp.dot(
                lhs, a_block[:, c * chunk : (c + 1) * chunk], preferred_element_type=F32
            )
            if c < along_x:
                for k in range(pairs):
                    to_x[c, k] = jnp.concatenate(
                        tile(product, k) + tile(product, pairs + k), axis=0
                    ).astype(BF16)
            else:
                n = c - along_x
                for k in range(2):
                    to_z[n, k] = jnp.concatenate(
                        sum([tile(product, k * pairs + m) for m in range(pairs)], []), axis=0
                    ).astype(BF16)
            launch(c)
        sent.append((out_x, from_x))
        sent.append((out_z, from_z))

    send_dense(
        residual_all[y], near_x, near_z, near_by_x, near_by_z, near_x_out, near_z_out, near_back
    )

    @pl.when(lead)
    def _():
        for n, yy in enumerate(y_from):
            slot = residual_all.at[yy]
            await_all(recv_sem, r_back[n], slot)
            remote(slot, slot, partner, pass_out, pass_back).start()

    pl.when(follow)(lambda: await_all(recv_sem, pass_back, residual_all.at[pl.ds(0, far - 1)]))
    send_dense(
        jnp.concatenate([residual_all[yy] for yy in y_from], axis=0),
        rest_x,
        rest_z,
        rest_by_x,
        rest_by_z,
        x_out,
        z_out,
        rest_back,
    )

    @pl.when(lead)
    def _():
        await_all(recv_sem, energy_back, energy_all.at[pl.ds(0, far - 1)])
        energy_sum[...] = jnp.sum(energy_all[...], axis=0)
        remote(energy_sum, energy_sum, partner, total_out, total_back).start()
        lead_sent.append((total_out, lambda: energy_sum))

    rest = part * (far - 1)
    second = {}
    pair_out, line_out = next(sending), next(sending)
    for c in order:
        second[c] = next(landing)
        if c < along_x:
            await_all(recv_sem, near_back[c], near_by_x.at[c])
            near = near_x[c, x].astype(F32) + jnp.sum(near_by_x[c].astype(F32), axis=0)
            await_all(recv_sem, rest_back[c], rest_by_x.at[c])
            total = rest_x[c, x].astype(F32) + jnp.sum(rest_by_x[c].astype(F32), axis=0)
            for k in range(2):
                pair_send[c, k] = jnp.concatenate(
                    [near[k * part :][:part], total[k * rest :][:rest]], axis=0
                ).astype(BF16)
            remote(
                pair_send.at[c, 1 - z], pair_recv.at[c], across, pair_out, second[c]
            ).start()
        else:
            n = c - along_x
            await_all(recv_sem, near_back[c], near_by_z.at[n])
            near = near_z[n, z].astype(F32) + near_by_z[n].astype(F32)
            await_all(recv_sem, rest_back[c], rest_by_z.at[n])
            total = rest_z[n, z].astype(F32) + rest_by_z[n].astype(F32)
            for k in range(pairs):
                line_send[n, k] = jnp.concatenate(
                    [near[k * part :][:part], total[k * rest :][:rest]], axis=0
                ).astype(BF16)
            for m, peer in enumerate(x_peers):
                remote(
                    line_send.at[n, lax.rem(peer[0], pairs)],
                    line_recv.at[n, m],
                    peer,
                    line_out,
                    second[c],
                ).start()
    sent.append((pair_out, pair_recv))
    sent.append((line_out, line_recv))

    pl.when(follow)(lambda: await_all(recv_sem, total_back, energy_sum))
    norm_all[i, :, width:] = energy_sum[...]
    pl.when(loop)(lambda: await_all(recv_sem, move_back, moved_recv.at[pl.ds(0, far - 1)]))
    pl.when(no_loop)(lambda: await_all(recv_sem, move_back, moved_recv))
    y_order = [y] + y_from
    moved = split3(jnp.concatenate([moved_recv[yy] for yy in y_order], axis=0))
    for c in order:
        span = slice(c * chunk, (c + 1) * chunk)
        before = add3(
            jnp.dot(
                moved,
                one_hot(index_own[steps - 2], c * chunk, chunk).astype(BF16),
                preferred_element_type=F32,
            )
        )
        mask = jnp.sum(one_hot(index_own[steps - 1], c * chunk, chunk), axis=0, keepdims=True)
        if c < along_x:
            await_all(recv_sem, second[c], pair_recv.at[c])
            gradient = pair_send[c, z].astype(F32) + pair_recv[c].astype(F32)
        else:
            n = c - along_x
            await_all(recv_sem, second[c], line_recv.at[n])
            gradient = line_send[n, x].astype(F32) + jnp.sum(line_recv[n].astype(F32), axis=0)
        stepped = before + STEP_SIZE * gradient
        settled = stepped * mask
        for n, yy in enumerate(y_order):
            kept_out[rows_of(0, yy), span] = settled[n * part : (n + 1) * part]
        norm_all[i, :, span] = jnp.sum(stepped * stepped, axis=0, keepdims=True)

    out, back = next(sending), next(landing)
    mine = norm_all.at[i]
    for peer in row_peers:
        remote(mine, mine, peer, out, back).start()
    others = norm_all.at[pl.ds(0, rows - 1)]
    sent.append((out, others))
    await_all(recv_sem, back, others)
    sums_out[...] = jnp.sum(norm_all[...], axis=0)

    pl.when(loop)(
        lambda: await_all(send_sem, first_out, first_send.at[pl.ds(0, far - 1)])
    )
    pl.when(no_loop)(lambda: await_all(send_sem, first_out, first_send))
    for out, ref in sent:
        await_all(send_sem, out, ref)

    @pl.when(lead)
    def _():
        for t in range(steps - 1):
            await_all(send_sem, kept_out_sem[t], kept.at[t, pl.ds(0, far - 1)])
        for k in range(rows):
            pl.when(jnp.logical_not(here[k]))(moves[k].wait_send)
        for out, ref in lead_sent:
            await_all(send_sem, out, ref())

    @pl.when(follow)
    def _():
        await_all(send_sem, kept_out_sem[steps - 2], kept.at[steps - 2, pl.ds(0, far)])


def finish(total_count, kept, sums, estimate, norms, energies):
    width = kept.shape[1]
    estimate[...] = kept[...]
    norms[...] = jnp.sqrt(sums[:, :width]).reshape(width)
    for t in range(energies.shape[0]):
        energies[t] = sums[0, width + t] / total_count


def solution(mesh, far=4, high=4, chunk=512, along_x=4):
    rows = mesh.shape["row"]

    def local(matrix, measured, support):
        depth, width = matrix.shape
        signals = measured.shape[0]
        group = signals // rows
        part = group // far
        party = rows * part
        rest = part * (far - 1)
        pairs = rows // 2
        steps = support.shape[0]
        turns = steps - 1
        span = min(chunk, width)
        chunks = width // span
        along_z = chunks - along_x
        in_vmem = pl.BlockSpec(memory_space=pltpu.VMEM)
        in_hbm = pl.BlockSpec(memory_space=pltpu.HBM)
        kept, sums = pl.pallas_call(
            functools.partial(kernel, (rows, far, high, along_x)),
            out_shape=(
                jax.ShapeDtypeStruct((group, width), F32),
                jax.ShapeDtypeStruct((1, width + KMAX), F32),
            ),
            in_specs=[in_hbm] * 3,
            out_specs=(in_vmem,) * 2,
            scratch_shapes=[
                pltpu.VMEM(support.shape, jnp.int32),
                pltpu.VMEM(measured.shape, F32),
                pltpu.VMEM((depth, width), BF16),
                pltpu.VMEM((steps, KMAX, 1), jnp.int32),
                pltpu.VMEM((turns, KMAX, 1), jnp.int32),
                pltpu.VMEM((turns, rows, KMAX, depth), BF16),
                pltpu.VMEM((far, party, KMAX), BF16),
                pltpu.VMEM((rows, party, KMAX), BF16),
                pltpu.VMEM((turns, rows, party, KMAX), BF16),
                pltpu.VMEM((turns, rows - 1, party, KMAX), BF16),
                pltpu.VMEM((turns, rows, party, KMAX), BF16),
                pltpu.VMEM((party, KMAX), F32),
                pltpu.VMEM((turns, high, party, depth), BF16),
                pltpu.VMEM((rows, part, KMAX), F32),
                pltpu.VMEM((far, part, KMAX), F32),
                pltpu.VMEM((far, party, depth), BF16),
                pltpu.VMEM((far, 1, KMAX), F32),
                pltpu.VMEM((1, KMAX), F32),
                pltpu.VMEM((along_x, pairs, 2 * part, span), BF16),
                pltpu.VMEM((along_z, 2, pairs * part, span), BF16),
                pltpu.VMEM((along_x, pairs - 1, 2 * part, span), BF16),
                pltpu.VMEM((along_z, pairs * part, span), BF16),
                pltpu.VMEM((along_x, pairs, 2 * rest, span), BF16),
                pltpu.VMEM((along_z, 2, pairs * rest, span), BF16),
                pltpu.VMEM((along_x, pairs - 1, 2 * rest, span), BF16),
                pltpu.VMEM((along_z, pairs * rest, span), BF16),
                pltpu.VMEM((along_x, 2, group, span), BF16),
                pltpu.VMEM((along_x, group, span), BF16),
                pltpu.VMEM((along_z, pairs, group, span), BF16),
                pltpu.VMEM((along_z, pairs - 1, group, span), BF16),
                pltpu.VMEM((rows, 1, width + KMAX), F32),
                pltpu.SemaphoreType.DMA((chunks + 2,)),
                pltpu.SemaphoreType.DMA((24,)),
                pltpu.SemaphoreType.DMA((21 + 3 * chunks,)),
            ],
            compiler_params=pltpu.CompilerParams(
                collective_id=0, has_side_effects=True, vmem_limit_bytes=40 * 2**20
            ),
        )(*(pltpu.with_memory_space_constraint(a, pltpu.HBM) for a in (support, measured, matrix)))
        return pl.pallas_call(
            functools.partial(finish, float(signals * depth * rows)),
            out_shape=(
                jax.ShapeDtypeStruct((group, width), F32),
                jax.ShapeDtypeStruct((width,), F32),
                jax.ShapeDtypeStruct((steps,), F32),
            ),
            in_specs=[in_vmem] * 2,
            out_specs=(in_vmem, in_vmem, pl.BlockSpec(memory_space=pltpu.SMEM)),
            compiler_params=pltpu.CompilerParams(vmem_limit_bytes=4 * 2**20),
        )(kept, sums)

    return jax.shard_map(
        local,
        mesh=mesh,
        in_specs=(P("row", "col"), P(None, "row"), P()),
        out_specs=(P("row", "col"), P("col"), P()),
        check_vma=False,
    )
```

```python
import functools

import jax
import jax.numpy as jnp
from jax import lax
from jax.experimental import pallas as pl
from jax.experimental.pallas import tpu as pltpu
from jax.sharding import PartitionSpec as P

KMAX = 128
STEP_SIZE = 0.25
CORES = 2
LEAD = 1
NEAR = (((1,), (1,)), ((), ()))
F32 = jnp.float32
BF16 = jnp.bfloat16


def iota(shape, dim):
    return lax.broadcasted_iota(jnp.int32, shape, dim)


def window(line, start, width):
    count = line.shape[1]
    below = jnp.sum(jnp.where(line < start, 1.0, 0.0), axis=1, keepdims=True)
    upto = jnp.sum(jnp.where(line < start + width, 1.0, 0.0), axis=1, keepdims=True)
    place = iota((KMAX, count), 1) - iota((KMAX, count), 0)
    local = (line - start).astype(F32)
    found = jnp.sum(
        jnp.where(place == below.astype(jnp.int32), local, 0.0), axis=1, keepdims=True
    )
    there = iota((KMAX, 1), 0).astype(F32) < upto - below
    return jnp.where(there, found, -1.0).astype(jnp.int32)


def one_hot(index, first, width):
    return jnp.where(iota((KMAX, width), 1) + first == index, 1.0, 0.0)


def split3(value):
    high = value.astype(BF16)
    rest = value - high.astype(F32)
    middle = rest.astype(BF16)
    low = (rest - middle.astype(F32)).astype(BF16)
    return jnp.concatenate([high, middle, low], axis=0)


def add3(value):
    third = value.shape[0] // 3
    return value[:third] + value[third : 2 * third] + value[2 * third :]


def kernel(
    shape,
    support_in,
    measured_in,
    matrix,
    kept_out,
    sums_out,
    support,
    measured,
    a_block,
    index_own,
    index_held,
    kept,
    turned,
    first_send,
    first_recv,
    slope_send,
    slope_recv,
    current_all,
    held,
    seen_all,
    moved_send,
    moved_recv,
    residual_all,
    energy_all,
    energy_sum,
    near_x,
    near_z,
    near_by_x,
    near_by_z,
    rest_x,
    rest_z,
    rest_by_x,
    rest_by_z,
    pair_send,
    pair_recv,
    line_send,
    line_recv,
    carry_all,
    mask_all,
    norm_all,
    load_sem,
    send_sem,
    recv_sem,
):
    rows, far, high, along_x = shape
    pairs = rows // 2
    depth, width = matrix.shape
    group = measured.shape[0] // rows
    part = group // far
    party = rows * part
    steps = support.shape[0]
    chunk = near_x.shape[3]
    chunks = width // chunk
    i = lax.axis_index("row")
    col = lax.axis_index("col")
    x = lax.rem(i, pairs)
    z = i // pairs
    core = lax.rem(col, CORES)
    h = lax.rem(col // CORES, high)
    y = col // (CORES * high)
    q = y * CORES + core
    lead = core == LEAD
    follow = core != LEAD
    sending = iter(range(send_sem.shape[0]))
    landing = iter(range(recv_sem.shape[0]))
    sent = []
    lead_sent = []

    def at(yy, hh, cc):
        return (yy * high + hh) * CORES + cc

    def member(k):
        return at(k // CORES, h, lax.rem(k, CORES))

    def far_first(count):
        return sorted(range(1, count), key=lambda d: -min(d, count - d))

    def remote(src, dst, where, out, back):
        return pltpu.make_async_remote_copy(
            src_ref=src,
            dst_ref=dst,
            send_sem=send_sem.at[out],
            recv_sem=recv_sem.at[back],
            device_id=where,
            device_id_type=pl.DeviceIdType.MESH,
        )

    def await_all(sems, slot, ref):
        pltpu.make_async_copy(ref, ref, sems.at[slot]).wait()

    x_shift = far_first(pairs)
    offsets = [(1, d) for d in x_shift] + [(0, d) for d in x_shift] + [(1, 0)]
    row_peers = [
        (lax.rem(z + dz, 2) * pairs + lax.rem(x + dx, pairs), col) for dz, dx in offsets
    ]
    x_peers = [(z * pairs + lax.rem(x + d, pairs), col) for d in x_shift]
    across = ((1 - z) * pairs + x, col)
    y_shift = far_first(far)
    y_near = [lax.rem(y + d, far) for d in y_shift]
    y_from = [lax.rem(y - d + far, far) for d in y_shift]
    y_leads = [(i, at(yy, h, LEAD)) for yy in y_near]
    h_peers = [(i, at(y, lax.rem(h + d, high), core)) for d in far_first(high)]
    partner = (i, at(y, h, 1 - core))
    def rows_of(k, yy):
        return pl.ds(pl.multiple_of(k * group + yy * part, part), part)

    support_load = pltpu.make_async_copy(support_in, support, load_sem.at[chunks])
    support_load.start()
    loads = [
        pltpu.make_async_copy(
            matrix.at[:, pl.ds(c * chunk, chunk)],
            a_block.at[:, pl.ds(c * chunk, chunk)],
            load_sem.at[c],
        )
        for c in range(chunks)
    ]
    for load in loads:
        load.start()
    measured_load = pltpu.make_async_copy(measured_in, measured, load_sem.at[chunks + 1])
    measured_load.start()
    barrier = pltpu.get_barrier_semaphore()

    def greet(peer):
        pl.semaphore_signal(
            barrier, inc=1, device_id=peer, device_id_type=pl.DeviceIdType.MESH
        )

    on_diagonal = i == q
    loop = jnp.logical_and(on_diagonal, lead)
    no_loop = jnp.logical_not(loop)

    @pl.when(lead)
    def _():
        for k in range(rows):
            pl.when(jnp.logical_or(jnp.logical_not(on_diagonal), i != k))(
                lambda k=k: greet((k, member(i)))
            )
        for peer in h_peers:
            greet(peer)

    for k in range(far):
        pl.when(jnp.logical_or(no_loop, y != k))(lambda k=k: greet((q, at(k, h, LEAD))))
    for peer in row_peers + [partner]:
        greet(peer)

    @pl.when(lead)
    def _():
        for yy in y_near:
            for cc in range(CORES):
                greet((i, at(yy, h, cc)))

    greetings = (
        len(row_peers) + 1 + len(y_leads) + far
        + jnp.where(lead, len(h_peers) + rows, 0)
        - jnp.where(loop, 2, 0)
    )

    support_load.wait()

    def find_own(t):
        index_own[t] = window(support[t : t + 1, :], col * width, width)

    def pick(first, last, loaded):
        total = jnp.zeros(((last - first) * KMAX, depth), F32)
        for c in range(chunks):
            if not loaded:
                loads[c].wait()
            hot = jnp.concatenate(
                [one_hot(index_own[t], c * chunk, chunk).astype(BF16) for t in range(first, last)],
                axis=0,
            )
            total += lax.dot_general(
                hot, a_block[:, c * chunk : (c + 1) * chunk], NEAR, preferred_element_type=F32
            )
        for t in range(first, last):
            kept[t, q] = total[(t - first) * KMAX : (t - first + 1) * KMAX, :].astype(BF16)

    find_own(0)
    pick(0, 1, False)
    measured_load.wait()

    first = lax.dot_general(
        measured[...].astype(BF16), kept[0, q], NEAR, preferred_element_type=F32
    )
    for n in range(far):
        first_send[n] = jnp.concatenate(
            [first[k * group + n * part :][:part] for k in range(rows)], axis=0
        ).astype(BF16)

    pl.semaphore_wait(barrier, greetings)

    first_out, first_back = next(sending), next(landing)
    for k in range(far):
        copy = remote(
            first_send.at[k], first_recv.at[i], (q, at(k, h, LEAD)), first_out, first_back
        )
        other = jnp.logical_or(no_loop, y != k)
        pl.when(other)(copy.start)

        @pl.when(jnp.logical_not(other))
        def _():
            first_recv[i] = first_send[k]

    kept_out_sem = [next(sending) for _ in range(steps - 1)]
    kept_back = [next(landing) for _ in range(steps - 1)]

    def spread(t):
        own = kept.at[t, q]
        for peer in y_leads:
            remote(own, own, peer, kept_out_sem[t], kept_back[t]).start()
        pl.when(follow)(lambda: remote(own, own, partner, kept_out_sem[t], kept_back[t]).start())

    spread(0)
    for t in range(1, steps - 1):
        find_own(t)
    pick(1, steps - 1, True)
    find_own(steps - 1)

    @pl.when(follow)
    def _():
        for t in range(1, steps - 1):
            await_all(send_sem, kept_out_sem[t - 1], kept.at[t - 1, pl.ds(0, far)])
            spread(t)


    def carried(t, value):
        diagonal = iota((KMAX, KMAX), 0) == iota((KMAX, KMAX), 1)
        after = jnp.sum(
            jnp.where(diagonal, index_held[t + 1].astype(F32), 0.0), axis=0, keepdims=True
        ).astype(jnp.int32)
        before = index_held[t]
        same = jnp.where(jnp.logical_and(before == after, before >= 0), 1.0, 0.0).astype(BF16)
        return add3(jnp.dot(split3(value), same, preferred_element_type=F32))

    move_out, move_back = next(sending), next(landing)
    energy_out, energy_back, total_out, total_back = (
        next(sending), next(landing), next(sending), next(landing)
    )
    r_out, r_back = next(sending), [next(landing) for _ in y_leads]
    pass_out, own_back, pass_back = next(sending), next(landing), next(landing)
    moves = [
        remote(moved_send.at[k], moved_recv.at[y], (k, member(i)), move_out, move_back)
        for k in range(rows)
    ]
    here = [jnp.logical_and(on_diagonal, i == k) for k in range(rows)]

    @pl.when(lead)
    def _():
        for t in range(steps - 1):
            index_held[t] = window(support[t : t + 1, :], member(i) * width, width)
        pl.when(on_diagonal)(
            lambda: await_all(recv_sem, first_back, first_recv.at[pl.ds(0, rows - 1)])
        )
        pl.when(jnp.logical_not(on_diagonal))(lambda: await_all(recv_sem, first_back, first_recv))
        current = STEP_SIZE * jnp.sum(first_recv[...].astype(F32), axis=0)

        own_measured = jnp.concatenate(
            [measured[rows_of(k, y), :] for k in range(rows)], axis=0
        )
        energy = [jnp.sum(own_measured * own_measured, axis=0, keepdims=True)]
        for t in range(steps - 1):
            if t > 0:
                slope = jnp.dot(
                    residual.astype(BF16), turned[t - 1], preferred_element_type=F32
                ).astype(BF16)
                for k in range(rows):
                    slope_send[t - 1, k] = slope[:, k * KMAX : (k + 1) * KMAX]
                out, back = next(sending), next(landing)
                for n, peer in enumerate(row_peers):
                    remote(
                        slope_send.at[t - 1, peer[0]], slope_recv.at[t - 1, n], peer, out, back
                    ).start()
                lead_sent.append((out, lambda t=t: slope_recv.at[t - 1]))
                carry = carried(t - 1, held[...])
                await_all(recv_sem, back, slope_recv.at[t - 1])
                gathered = slope_send[t - 1, i].astype(F32) + jnp.sum(
                    slope_recv[t - 1].astype(F32), axis=0
                )
                current = carry + STEP_SIZE * gathered
            held[...] = current
            current_all[t, i] = current.astype(BF16)
            out, back = next(sending), next(landing)
            mine = current_all.at[t, i]
            for peer in row_peers:
                remote(mine, mine, peer, out, back).start()
            others = current_all.at[t, pl.ds(0, rows - 1)]
            lead_sent.append((out, lambda t=t: current_all.at[t, pl.ds(0, rows - 1)]))
            if t == steps - 2:
                for k in range(rows):
                    moved_send[k] = current[k * part : (k + 1) * part, :]
                    pl.when(jnp.logical_not(here[k]))(moves[k].start)

                    @pl.when(here[k])
                    def _():
                        moved_recv[y] = moved_send[k]

            if t < steps - 2:
                spread(t + 1)
            if t == 0:
                await_all(recv_sem, kept_back[t], kept.at[t, pl.ds(0, rows - 1)])
            await_all(recv_sem, back, others)
            signals = jnp.concatenate([current_all[t, k] for k in range(rows)], axis=1)
            seen_all[t, h] = jnp.dot(
                signals, kept[t].reshape(rows * KMAX, depth), preferred_element_type=F32
            ).astype(BF16)
            out, back = next(sending), next(landing)
            mine = seen_all.at[t, h]
            for peer in h_peers:
                remote(mine, mine, peer, out, back).start()
            others = seen_all.at[t, pl.ds(0, high - 1)]
            lead_sent.append((out, lambda t=t: seen_all.at[t, pl.ds(0, high - 1)]))
            if t < steps - 2:
                await_all(recv_sem, kept_back[t + 1], kept.at[t + 1, pl.ds(0, rows - 1)])
                turned[t] = kept[t + 1].reshape(rows * KMAX, depth).T
            await_all(recv_sem, back, others)
            residual = own_measured - jnp.sum(seen_all[t].astype(F32), axis=0)
            energy.append(jnp.sum(residual * residual, axis=0, keepdims=True))

        residual_all[y] = residual.astype(BF16)
        own = residual_all.at[y]
        for n, peer in enumerate(y_leads):
            remote(own, own, peer, r_out, r_back[n]).start()
        remote(own, own, partner, pass_out, own_back).start()
        lanes = iota((1, KMAX), 1)
        values = jnp.zeros((1, KMAX), F32)
        for t in range(steps):
            values = jnp.where(lanes == t, jnp.sum(energy[t], axis=1, keepdims=True), values)
        energy_all[y] = values
        mine = energy_all.at[y]
        for peer in y_leads:
            remote(mine, mine, peer, energy_out, energy_back).start()
        lead_sent.append((r_out, lambda: residual_all.at[pl.ds(0, far - 1)]))
        lead_sent.append((pass_out, lambda: residual_all))
        lead_sent.append((energy_out, lambda: energy_all.at[pl.ds(0, far - 1)]))

    pl.when(follow)(lambda: await_all(recv_sem, own_back, residual_all.at[0]))

    z_out, x_out, near_z_out, near_x_out = (next(sending) for _ in range(4))
    near_back = [next(landing) for _ in range(chunks)]
    first_by_x = list(range(along_x))
    across_first = list(range(along_x, chunks))
    order = []
    for n in range(max(len(first_by_x), len(across_first))):
        pair = first_by_x[n : n + 1] + across_first[n : n + 1]
        order += pair if n == 0 else pair[::-1]

    def send_dense(lhs, to_x, to_z, from_x, from_z, out_x, out_z, back):
        count = lhs.shape[0] // party

        def launch(c):
            if c < along_x:
                for n, peer in enumerate(x_peers):
                    remote(
                        to_x.at[c, lax.rem(peer[0], pairs)], from_x.at[c, n], peer, out_x, back[c]
                    ).start()
            else:
                n = c - along_x
                remote(to_z.at[n, 1 - z], from_z.at[n], across, out_z, back[c]).start()

        def tile(product, k):
            return [product[n * party + k * part :][:part] for n in range(count)]

        for c in order:
            product = jnp.dot(
                lhs, a_block[:, c * chunk : (c + 1) * chunk], preferred_element_type=F32
            )
            if c < along_x:
                for k in range(pairs):
                    to_x[c, k] = jnp.concatenate(
                        tile(product, k) + tile(product, pairs + k), axis=0
                    ).astype(BF16)
            else:
                n = c - along_x
                for k in range(2):
                    to_z[n, k] = jnp.concatenate(
                        sum([tile(product, k * pairs + m) for m in range(pairs)], []), axis=0
                    ).astype(BF16)
            launch(c)
        sent.append((out_x, from_x))
        sent.append((out_z, from_z))

    send_dense(
        residual_all[y], near_x, near_z, near_by_x, near_by_z, near_x_out, near_z_out, near_back
    )

    pl.when(loop)(lambda: await_all(recv_sem, move_back, moved_recv.at[pl.ds(0, far - 1)]))
    pl.when(no_loop)(lambda: await_all(recv_sem, move_back, moved_recv))
    y_order = [y] + y_from
    moved = split3(jnp.concatenate([moved_recv[yy] for yy in y_order], axis=0))
    for c in order:
        span = slice(c * chunk, (c + 1) * chunk)
        carry_all[:, span] = add3(
            jnp.dot(
                moved,
                one_hot(index_own[steps - 2], c * chunk, chunk).astype(BF16),
                preferred_element_type=F32,
            )
        )
        mask_all[:, span] = jnp.sum(
            one_hot(index_own[steps - 1], c * chunk, chunk), axis=0, keepdims=True
        )

    @pl.when(lead)
    def _():
        for n, yy in enumerate(y_from):
            slot = residual_all.at[yy]
            await_all(recv_sem, r_back[n], slot)
            remote(slot, slot, partner, pass_out, pass_back).start()

    pl.when(follow)(lambda: await_all(recv_sem, pass_back, residual_all.at[pl.ds(0, far - 1)]))
    send_dense(
        jnp.concatenate([residual_all[yy] for yy in y_from], axis=0),
        rest_x,
        rest_z,
        rest_by_x,
        rest_by_z,
        x_out,
        z_out,
        near_back,
    )

    @pl.when(lead)
    def _():
        await_all(recv_sem, energy_back, energy_all.at[pl.ds(0, far - 1)])
        energy_sum[...] = jnp.sum(energy_all[...], axis=0)
        remote(energy_sum, energy_sum, partner, total_out, total_back).start()
        lead_sent.append((total_out, lambda: energy_sum))

    rest = part * (far - 1)
    both_x = kept_out.at[pl.ds(0, group), pl.ds(0, (pairs - 1) * chunk)]
    both_z = kept_out.at[pl.ds(0, group), pl.ds(0, pairs * chunk // 2)]
    second = {}
    pair_out, line_out = next(sending), next(sending)
    for c in order:
        second[c] = next(landing)
        if c < along_x:
            await_all(recv_sem, near_back[c], both_x)
            near = near_x[c, x].astype(F32) + jnp.sum(near_by_x[c].astype(F32), axis=0)
            total = rest_x[c, x].astype(F32) + jnp.sum(rest_by_x[c].astype(F32), axis=0)
            for k in range(2):
                pair_send[c, k] = jnp.concatenate(
                    [near[k * part :][:part], total[k * rest :][:rest]], axis=0
                ).astype(BF16)
            remote(
                pair_send.at[c, 1 - z], pair_recv.at[c], across, pair_out, second[c]
            ).start()
        else:
            n = c - along_x
            await_all(recv_sem, near_back[c], both_z)
            near = near_z[n, z].astype(F32) + near_by_z[n].astype(F32)
            total = rest_z[n, z].astype(F32) + rest_by_z[n].astype(F32)
            for k in range(pairs):
                line_send[n, k] = jnp.concatenate(
                    [near[k * part :][:part], total[k * rest :][:rest]], axis=0
                ).astype(BF16)
            for m, peer in enumerate(x_peers):
                remote(
                    line_send.at[n, lax.rem(peer[0], pairs)],
                    line_recv.at[n, m],
                    peer,
                    line_out,
                    second[c],
                ).start()
    sent.append((pair_out, pair_recv))
    sent.append((line_out, line_recv))

    norm_out, norm_back = [next(sending) for _ in range(2)], [next(landing) for _ in range(2)]
    early = max(chunks - 2, 1) * chunk
    spans = [pl.ds(0, early), pl.ds(early, width + KMAX - early)]

    def share(n):
        mine = norm_all.at[i, :, spans[n]]
        for peer in row_peers:
            remote(mine, mine, peer, norm_out[n], norm_back[n]).start()

    for place, c in enumerate(order):
        span = slice(c * chunk, (c + 1) * chunk)
        if c < along_x:
            await_all(recv_sem, second[c], pair_recv.at[c])
            gradient = pair_send[c, z].astype(F32) + pair_recv[c].astype(F32)
        else:
            n = c - along_x
            await_all(recv_sem, second[c], line_recv.at[n])
            gradient = line_send[n, x].astype(F32) + jnp.sum(line_recv[n].astype(F32), axis=0)
        stepped = carry_all[:, span] + STEP_SIZE * gradient
        norm_all[i, :, place * chunk : (place + 1) * chunk] = jnp.sum(
            stepped * stepped, axis=0, keepdims=True
        )
        if place == chunks - 1:
            pl.when(follow)(lambda: await_all(recv_sem, total_back, energy_sum))
            norm_all[i, :, width:] = energy_sum[...]
            share(1)
        elif (place + 1) * chunk == early:
            share(0)
        settled = stepped * mask_all[:, span]
        for n, yy in enumerate(y_order):
            kept_out[rows_of(0, yy), span] = settled[n * part : (n + 1) * part]

    for n in range(2):
        others = norm_all.at[pl.ds(0, rows - 1), :, spans[n]]
        sent.append((norm_out[n], others))
        await_all(recv_sem, norm_back[n], others)
    summed = jnp.sum(norm_all[...], axis=0)
    for place, c in enumerate(order):
        sums_out[:, c * chunk : (c + 1) * chunk] = summed[:, place * chunk : (place + 1) * chunk]
    sums_out[:, width:] = summed[:, width:]

    pl.when(loop)(
        lambda: await_all(send_sem, first_out, first_send.at[pl.ds(0, far - 1)])
    )
    pl.when(no_loop)(lambda: await_all(send_sem, first_out, first_send))
    for out, ref in sent:
        await_all(send_sem, out, ref)

    @pl.when(lead)
    def _():
        for t in range(steps - 1):
            await_all(send_sem, kept_out_sem[t], kept.at[t, pl.ds(0, far - 1)])
        for k in range(rows):
            pl.when(jnp.logical_not(here[k]))(moves[k].wait_send)
        for out, ref in lead_sent:
            await_all(send_sem, out, ref())

    @pl.when(follow)
    def _():
        await_all(send_sem, kept_out_sem[steps - 2], kept.at[steps - 2, pl.ds(0, far)])


def finish(total_count, kept, sums, estimate, norms, energies):
    width = kept.shape[1]
    estimate[...] = kept[...]
    norms[...] = jnp.sqrt(sums[:, :width]).reshape(width)
    for t in range(energies.shape[0]):
        energies[t] = sums[0, width + t] / total_count


def solution(mesh, far=4, high=4, chunk=512, along_x=4):
    rows = mesh.shape["row"]

    def local(matrix, measured, support):
        depth, width = matrix.shape
        signals = measured.shape[0]
        group = signals // rows
        part = group // far
        party = rows * part
        rest = part * (far - 1)
        pairs = rows // 2
        steps = support.shape[0]
        turns = steps - 1
        span = min(chunk, width)
        chunks = width // span
        along_z = chunks - along_x
        in_vmem = pl.BlockSpec(memory_space=pltpu.VMEM)
        in_hbm = pl.BlockSpec(memory_space=pltpu.HBM)
        kept, sums = pl.pallas_call(
            functools.partial(kernel, (rows, far, high, along_x)),
            out_shape=(
                jax.ShapeDtypeStruct((group, width), F32),
                jax.ShapeDtypeStruct((1, width + KMAX), F32),
            ),
            in_specs=[in_hbm] * 3,
            out_specs=(in_vmem,) * 2,
            scratch_shapes=[
                pltpu.VMEM(support.shape, jnp.int32),
                pltpu.VMEM(measured.shape, F32),
                pltpu.VMEM((depth, width), BF16),
                pltpu.VMEM((steps, KMAX, 1), jnp.int32),
                pltpu.VMEM((turns, KMAX, 1), jnp.int32),
                pltpu.VMEM((turns, rows, KMAX, depth), BF16),
                pltpu.VMEM((turns - 1, depth, rows * KMAX), BF16),
                pltpu.VMEM((far, party, KMAX), BF16),
                pltpu.VMEM((rows, party, KMAX), BF16),
                pltpu.VMEM((turns, rows, party, KMAX), BF16),
                pltpu.VMEM((turns, rows - 1, party, KMAX), BF16),
                pltpu.VMEM((turns, rows, party, KMAX), BF16),
                pltpu.VMEM((party, KMAX), F32),
                pltpu.VMEM((turns, high, party, depth), BF16),
                pltpu.VMEM((rows, part, KMAX), F32),
                pltpu.VMEM((far, part, KMAX), F32),
                pltpu.VMEM((far, party, depth), BF16),
                pltpu.VMEM((far, 1, KMAX), F32),
                pltpu.VMEM((1, KMAX), F32),
                pltpu.VMEM((along_x, pairs, 2 * part, span), BF16),
                pltpu.VMEM((along_z, 2, pairs * part, span), BF16),
                pltpu.VMEM((along_x, pairs - 1, 2 * part, span), BF16),
                pltpu.VMEM((along_z, pairs * part, span), BF16),
                pltpu.VMEM((along_x, pairs, 2 * rest, span), BF16),
                pltpu.VMEM((along_z, 2, pairs * rest, span), BF16),
                pltpu.VMEM((along_x, pairs - 1, 2 * rest, span), BF16),
                pltpu.VMEM((along_z, pairs * rest, span), BF16),
                pltpu.VMEM((along_x, 2, group, span), BF16),
                pltpu.VMEM((along_x, group, span), BF16),
                pltpu.VMEM((along_z, pairs, group, span), BF16),
                pltpu.VMEM((along_z, pairs - 1, group, span), BF16),
                pltpu.VMEM((group, width), F32),
                pltpu.VMEM((1, width), F32),
                pltpu.VMEM((rows, 1, width + KMAX), F32),
                pltpu.SemaphoreType.DMA((chunks + 2,)),
                pltpu.SemaphoreType.DMA((25,)),
                pltpu.SemaphoreType.DMA((22 + 2 * chunks,)),
            ],
            compiler_params=pltpu.CompilerParams(
                collective_id=0, has_side_effects=True, vmem_limit_bytes=40 * 2**20
            ),
        )(*(pltpu.with_memory_space_constraint(a, pltpu.HBM) for a in (support, measured, matrix)))
        return pl.pallas_call(
            functools.partial(finish, float(signals * depth * rows)),
            out_shape=(
                jax.ShapeDtypeStruct((group, width), F32),
                jax.ShapeDtypeStruct((width,), F32),
                jax.ShapeDtypeStruct((steps,), F32),
            ),
            in_specs=[in_vmem] * 2,
            out_specs=(in_vmem, in_vmem, pl.BlockSpec(memory_space=pltpu.SMEM)),
            compiler_params=pltpu.CompilerParams(vmem_limit_bytes=4 * 2**20),
        )(kept, sums)

    return jax.shard_map(
        local,
        mesh=mesh,
        in_specs=(P("row", "col"), P(None, "row"), P()),
        out_specs=(P("row", "col"), P("col"), P()),
        check_vma=False,
    )
```

```python
import functools

import jax
import jax.numpy as jnp
from jax import lax
from jax.experimental import pallas as pl
from jax.experimental.pallas import tpu as pltpu
from jax.sharding import PartitionSpec as P

KMAX = 128
STEP_SIZE = 0.25
CORES = 2
LEAD = 1
NEAR = (((1,), (1,)), ((), ()))
F32 = jnp.float32
BF16 = jnp.bfloat16


def iota(shape, dim):
    return lax.broadcasted_iota(jnp.int32, shape, dim)


def window(line, start, width):
    count = line.shape[1]
    below = jnp.sum(jnp.where(line < start, 1.0, 0.0), axis=1, keepdims=True)
    upto = jnp.sum(jnp.where(line < start + width, 1.0, 0.0), axis=1, keepdims=True)
    place = iota((KMAX, count), 1) - iota((KMAX, count), 0)
    local = (line - start).astype(F32)
    found = jnp.sum(
        jnp.where(place == below.astype(jnp.int32), local, 0.0), axis=1, keepdims=True
    )
    there = iota((KMAX, 1), 0).astype(F32) < upto - below
    return jnp.where(there, found, -1.0).astype(jnp.int32)


def one_hot(index, first, width):
    return jnp.where(iota((KMAX, width), 1) + first == index, 1.0, 0.0)


def split3(value):
    high = value.astype(BF16)
    rest = value - high.astype(F32)
    middle = rest.astype(BF16)
    low = (rest - middle.astype(F32)).astype(BF16)
    return jnp.concatenate([high, middle, low], axis=0)


def add3(value):
    third = value.shape[0] // 3
    return value[:third] + value[third : 2 * third] + value[2 * third :]


def kernel(
    shape,
    support_in,
    measured_in,
    matrix,
    kept_out,
    sums_out,
    support,
    measured,
    a_block,
    index_own,
    index_held,
    kept,
    turned,
    first_send,
    first_recv,
    slope_send,
    slope_recv,
    current_all,
    held,
    seen_all,
    moved_send,
    moved_recv,
    residual_all,
    energy_all,
    energy_sum,
    near_x,
    near_z,
    near_by_x,
    near_by_z,
    rest_x,
    rest_z,
    rest_by_x,
    rest_by_z,
    pair_send,
    pair_recv,
    line_send,
    line_recv,
    carry_all,
    mask_all,
    norm_all,
    load_sem,
    send_sem,
    recv_sem,
):
    rows, far, high, along_x = shape
    pairs = rows // 2
    depth, width = matrix.shape
    group = measured.shape[0] // rows
    part = group // far
    party = rows * part
    steps = support.shape[0]
    chunk = near_x.shape[3]
    chunks = width // chunk
    i = lax.axis_index("row")
    col = lax.axis_index("col")
    x = lax.rem(i, pairs)
    z = i // pairs
    core = lax.rem(col, CORES)
    h = lax.rem(col // CORES, high)
    y = col // (CORES * high)
    q = y * CORES + core
    lead = core == LEAD
    follow = core != LEAD
    sending = iter(range(send_sem.shape[0]))
    landing = iter(range(recv_sem.shape[0]))
    sent = []
    lead_sent = []

    def at(yy, hh, cc):
        return (yy * high + hh) * CORES + cc

    def member(k):
        return at(k // CORES, h, lax.rem(k, CORES))

    def far_first(count):
        return sorted(range(1, count), key=lambda d: -min(d, count - d))

    def remote(src, dst, where, out, back):
        return pltpu.make_async_remote_copy(
            src_ref=src,
            dst_ref=dst,
            send_sem=send_sem.at[out],
            recv_sem=recv_sem.at[back],
            device_id=where,
            device_id_type=pl.DeviceIdType.MESH,
        )

    def await_all(sems, slot, ref):
        pltpu.make_async_copy(ref, ref, sems.at[slot]).wait()

    x_shift = far_first(pairs)
    offsets = [(1, d) for d in x_shift] + [(0, d) for d in x_shift] + [(1, 0)]
    row_peers = [
        (lax.rem(z + dz, 2) * pairs + lax.rem(x + dx, pairs), col) for dz, dx in offsets
    ]
    x_peers = [(z * pairs + lax.rem(x + d, pairs), col) for d in x_shift]
    across = ((1 - z) * pairs + x, col)
    y_shift = far_first(far)
    y_near = [lax.rem(y + d, far) for d in y_shift]
    y_from = [lax.rem(y - d + far, far) for d in y_shift]
    y_leads = [(i, at(yy, h, LEAD)) for yy in y_near]
    h_peers = [(i, at(y, lax.rem(h + d, high), core)) for d in far_first(high)]
    partner = (i, at(y, h, 1 - core))
    def rows_of(k, yy):
        return pl.ds(pl.multiple_of(k * group + yy * part, part), part)

    support_load = pltpu.make_async_copy(support_in, support, load_sem.at[chunks])
    support_load.start()
    loads = [
        pltpu.make_async_copy(
            matrix.at[:, pl.ds(c * chunk, chunk)],
            a_block.at[:, pl.ds(c * chunk, chunk)],
            load_sem.at[c],
        )
        for c in range(chunks)
    ]
    for load in loads:
        load.start()
    measured_load = pltpu.make_async_copy(measured_in, measured, load_sem.at[chunks + 1])
    measured_load.start()
    barrier = pltpu.get_barrier_semaphore()

    def greet(peer):
        pl.semaphore_signal(
            barrier, inc=1, device_id=peer, device_id_type=pl.DeviceIdType.MESH
        )

    on_diagonal = i == q
    loop = jnp.logical_and(on_diagonal, lead)
    no_loop = jnp.logical_not(loop)

    @pl.when(lead)
    def _():
        for k in range(rows):
            pl.when(jnp.logical_or(jnp.logical_not(on_diagonal), i != k))(
                lambda k=k: greet((k, member(i)))
            )
        for peer in h_peers:
            greet(peer)

    for k in range(far):
        pl.when(jnp.logical_or(no_loop, y != k))(lambda k=k: greet((q, at(k, h, LEAD))))
    for peer in row_peers + [partner]:
        greet(peer)

    @pl.when(lead)
    def _():
        for yy in y_near:
            for cc in range(CORES):
                greet((i, at(yy, h, cc)))

    greetings = (
        len(row_peers) + 1 + len(y_leads) + far
        + jnp.where(lead, len(h_peers) + rows, 0)
        - jnp.where(loop, 2, 0)
    )

    support_load.wait()

    def find_own(t):
        index_own[t] = window(support[t : t + 1, :], col * width, width)

    def pick(first, last, loaded):
        total = jnp.zeros(((last - first) * KMAX, depth), F32)
        for c in range(chunks):
            if not loaded:
                loads[c].wait()
            hot = jnp.concatenate(
                [one_hot(index_own[t], c * chunk, chunk).astype(BF16) for t in range(first, last)],
                axis=0,
            )
            total += lax.dot_general(
                hot, a_block[:, c * chunk : (c + 1) * chunk], NEAR, preferred_element_type=F32
            )
        for t in range(first, last):
            kept[t, q] = total[(t - first) * KMAX : (t - first + 1) * KMAX, :].astype(BF16)

    find_own(0)
    pick(0, 1, False)
    measured_load.wait()

    first = lax.dot_general(
        measured[...].astype(BF16), kept[0, q], NEAR, preferred_element_type=F32
    )
    for n in range(far):
        first_send[n] = jnp.concatenate(
            [first[k * group + n * part :][:part] for k in range(rows)], axis=0
        ).astype(BF16)

    pl.semaphore_wait(barrier, greetings)

    first_out, first_back = next(sending), next(landing)
    for k in range(far):
        copy = remote(
            first_send.at[k], first_recv.at[i], (q, at(k, h, LEAD)), first_out, first_back
        )
        other = jnp.logical_or(no_loop, y != k)
        pl.when(other)(copy.start)

        @pl.when(jnp.logical_not(other))
        def _():
            first_recv[i] = first_send[k]

    kept_out_sem = [next(sending) for _ in range(steps - 1)]
    kept_back = [next(landing) for _ in range(steps - 1)]

    def spread(t):
        own = kept.at[t, q]
        for peer in y_leads[::-1]:
            remote(own, own, peer, kept_out_sem[t], kept_back[t]).start()
        pl.when(follow)(lambda: remote(own, own, partner, kept_out_sem[t], kept_back[t]).start())

    spread(0)
    for t in range(1, steps - 1):
        find_own(t)
    pick(1, steps - 1, True)
    find_own(steps - 1)

    @pl.when(follow)
    def _():
        for t in range(1, steps - 1):
            await_all(send_sem, kept_out_sem[t - 1], kept.at[t - 1, pl.ds(0, far)])
            spread(t)


    def carried(t, value):
        diagonal = iota((KMAX, KMAX), 0) == iota((KMAX, KMAX), 1)
        after = jnp.sum(
            jnp.where(diagonal, index_held[t + 1].astype(F32), 0.0), axis=0, keepdims=True
        ).astype(jnp.int32)
        before = index_held[t]
        same = jnp.where(jnp.logical_and(before == after, before >= 0), 1.0, 0.0).astype(BF16)
        return add3(jnp.dot(split3(value), same, preferred_element_type=F32))

    move_out, move_back = next(sending), next(landing)
    energy_out, energy_back, total_out, total_back = (
        next(sending), next(landing), next(sending), next(landing)
    )
    r_out, r_back = next(sending), [next(landing) for _ in y_leads]
    pass_out, own_back, pass_back = next(sending), next(landing), next(landing)
    moves = [
        remote(moved_send.at[k], moved_recv.at[y], (k, member(i)), move_out, move_back)
        for k in range(rows)
    ]
    here = [jnp.logical_and(on_diagonal, i == k) for k in range(rows)]

    @pl.when(lead)
    def _():
        for t in range(steps - 1):
            index_held[t] = window(support[t : t + 1, :], member(i) * width, width)
        pl.when(on_diagonal)(
            lambda: await_all(recv_sem, first_back, first_recv.at[pl.ds(0, rows - 1)])
        )
        pl.when(jnp.logical_not(on_diagonal))(lambda: await_all(recv_sem, first_back, first_recv))
        current = STEP_SIZE * jnp.sum(first_recv[...].astype(F32), axis=0)

        own_measured = jnp.concatenate(
            [measured[rows_of(k, y), :] for k in range(rows)], axis=0
        )
        energy = [jnp.sum(own_measured * own_measured, axis=0, keepdims=True)]
        for t in range(steps - 1):
            if t > 0:
                slope = jnp.dot(
                    residual.astype(BF16), turned[t - 1], preferred_element_type=F32
                ).astype(BF16)
                for k in range(rows):
                    slope_send[t - 1, k] = slope[:, k * KMAX : (k + 1) * KMAX]
                out, back = next(sending), next(landing)
                for n, peer in enumerate(row_peers):
                    remote(
                        slope_send.at[t - 1, peer[0]], slope_recv.at[t - 1, n], peer, out, back
                    ).start()
                lead_sent.append((out, lambda t=t: slope_recv.at[t - 1]))
                carry = carried(t - 1, held[...])
                await_all(recv_sem, back, slope_recv.at[t - 1])
                gathered = slope_send[t - 1, i].astype(F32) + jnp.sum(
                    slope_recv[t - 1].astype(F32), axis=0
                )
                current = carry + STEP_SIZE * gathered
            held[...] = current
            current_all[t, i] = current.astype(BF16)
            out, back = next(sending), next(landing)
            mine = current_all.at[t, i]
            for peer in row_peers:
                remote(mine, mine, peer, out, back).start()
            others = current_all.at[t, pl.ds(0, rows - 1)]
            lead_sent.append((out, lambda t=t: current_all.at[t, pl.ds(0, rows - 1)]))
            if t == steps - 2:
                for k in range(rows):
                    moved_send[k] = current[k * part : (k + 1) * part, :]
                    pl.when(jnp.logical_not(here[k]))(moves[k].start)

                    @pl.when(here[k])
                    def _():
                        moved_recv[y] = moved_send[k]

            if t < steps - 2:
                spread(t + 1)
            if t == 0:
                await_all(recv_sem, kept_back[t], kept.at[t, pl.ds(0, rows - 1)])
            await_all(recv_sem, back, others)
            signals = jnp.concatenate([current_all[t, k] for k in range(rows)], axis=1)
            seen_all[t, h] = jnp.dot(
                signals, kept[t].reshape(rows * KMAX, depth), preferred_element_type=F32
            ).astype(BF16)
            out, back = next(sending), next(landing)
            mine = seen_all.at[t, h]
            for peer in h_peers:
                remote(mine, mine, peer, out, back).start()
            others = seen_all.at[t, pl.ds(0, high - 1)]
            lead_sent.append((out, lambda t=t: seen_all.at[t, pl.ds(0, high - 1)]))
            if t < steps - 2:
                await_all(recv_sem, kept_back[t + 1], kept.at[t + 1, pl.ds(0, rows - 1)])
                turned[t] = kept[t + 1].reshape(rows * KMAX, depth).T
            await_all(recv_sem, back, others)
            residual = own_measured - jnp.sum(seen_all[t].astype(F32), axis=0)
            energy.append(jnp.sum(residual * residual, axis=0, keepdims=True))

        residual_all[y] = residual.astype(BF16)
        own = residual_all.at[y]
        for n, peer in enumerate(y_leads):
            remote(own, own, peer, r_out, r_back[n]).start()
        remote(own, own, partner, pass_out, own_back).start()
        lanes = iota((1, KMAX), 1)
        values = jnp.zeros((1, KMAX), F32)
        for t in range(steps):
            values = jnp.where(lanes == t, jnp.sum(energy[t], axis=1, keepdims=True), values)
        energy_all[y] = values
        mine = energy_all.at[y]
        for peer in y_leads:
            remote(mine, mine, peer, energy_out, energy_back).start()
        lead_sent.append((r_out, lambda: residual_all.at[pl.ds(0, far - 1)]))
        lead_sent.append((pass_out, lambda: residual_all))
        lead_sent.append((energy_out, lambda: energy_all.at[pl.ds(0, far - 1)]))

    pl.when(follow)(lambda: await_all(recv_sem, own_back, residual_all.at[0]))

    z_out, x_out, near_z_out, near_x_out = (next(sending) for _ in range(4))
    near_back = [next(landing) for _ in range(chunks)]
    first_by_x = list(range(along_x))
    across_first = list(range(along_x, chunks))
    order = []
    for n in range(max(len(first_by_x), len(across_first))):
        pair = first_by_x[n : n + 1] + across_first[n : n + 1]
        order += pair if n == 0 else pair[::-1]

    def send_dense(lhs, to_x, to_z, from_x, from_z, out_x, out_z, back):
        count = lhs.shape[0] // party

        def launch(c):
            if c < along_x:
                for n, peer in enumerate(x_peers):
                    remote(
                        to_x.at[c, lax.rem(peer[0], pairs)], from_x.at[c, n], peer, out_x, back[c]
                    ).start()
            else:
                n = c - along_x
                remote(to_z.at[n, 1 - z], from_z.at[n], across, out_z, back[c]).start()

        def tile(product, k):
            return [product[n * party + k * part :][:part] for n in range(count)]

        for c in order:
            product = jnp.dot(
                lhs, a_block[:, c * chunk : (c + 1) * chunk], preferred_element_type=F32
            )
            if c < along_x:
                for k in range(pairs):
                    to_x[c, k] = jnp.concatenate(
                        tile(product, k) + tile(product, pairs + k), axis=0
                    ).astype(BF16)
            else:
                n = c - along_x
                for k in range(2):
                    to_z[n, k] = jnp.concatenate(
                        sum([tile(product, k * pairs + m) for m in range(pairs)], []), axis=0
                    ).astype(BF16)
            launch(c)
        sent.append((out_x, from_x))
        sent.append((out_z, from_z))

    send_dense(
        residual_all[y], near_x, near_z, near_by_x, near_by_z, near_x_out, near_z_out, near_back
    )

    pl.when(loop)(lambda: await_all(recv_sem, move_back, moved_recv.at[pl.ds(0, far - 1)]))
    pl.when(no_loop)(lambda: await_all(recv_sem, move_back, moved_recv))
    y_order = [y] + y_from
    moved = split3(jnp.concatenate([moved_recv[yy] for yy in y_order], axis=0))
    for c in order:
        span = slice(c * chunk, (c + 1) * chunk)
        carry_all[:, span] = add3(
            jnp.dot(
                moved,
                one_hot(index_own[steps - 2], c * chunk, chunk).astype(BF16),
                preferred_element_type=F32,
            )
        )
        mask_all[:, span] = jnp.sum(
            one_hot(index_own[steps - 1], c * chunk, chunk), axis=0, keepdims=True
        )

    @pl.when(lead)
    def _():
        for n, yy in enumerate(y_from):
            slot = residual_all.at[yy]
            await_all(recv_sem, r_back[n], slot)
            remote(slot, slot, partner, pass_out, pass_back).start()

    pl.when(follow)(lambda: await_all(recv_sem, pass_back, residual_all.at[pl.ds(0, far - 1)]))
    send_dense(
        jnp.concatenate([residual_all[yy] for yy in y_from], axis=0),
        rest_x,
        rest_z,
        rest_by_x,
        rest_by_z,
        x_out,
        z_out,
        near_back,
    )

    @pl.when(lead)
    def _():
        await_all(recv_sem, energy_back, energy_all.at[pl.ds(0, far - 1)])
        energy_sum[...] = jnp.sum(energy_all[...], axis=0)
        remote(energy_sum, energy_sum, partner, total_out, total_back).start()
        lead_sent.append((total_out, lambda: energy_sum))

    rest = part * (far - 1)
    both_x = kept_out.at[pl.ds(0, group), pl.ds(0, (pairs - 1) * chunk)]
    both_z = kept_out.at[pl.ds(0, group), pl.ds(0, pairs * chunk // 2)]
    second = {}
    pair_out, line_out = next(sending), next(sending)
    for c in order:
        second[c] = next(landing)
        if c < along_x:
            await_all(recv_sem, near_back[c], both_x)
            near = near_x[c, x].astype(F32) + jnp.sum(near_by_x[c].astype(F32), axis=0)
            total = rest_x[c, x].astype(F32) + jnp.sum(rest_by_x[c].astype(F32), axis=0)
            for k in range(2):
                pair_send[c, k] = jnp.concatenate(
                    [near[k * part :][:part], total[k * rest :][:rest]], axis=0
                ).astype(BF16)
            remote(
                pair_send.at[c, 1 - z], pair_recv.at[c], across, pair_out, second[c]
            ).start()
        else:
            n = c - along_x
            await_all(recv_sem, near_back[c], both_z)
            near = near_z[n, z].astype(F32) + near_by_z[n].astype(F32)
            total = rest_z[n, z].astype(F32) + rest_by_z[n].astype(F32)
            for k in range(pairs):
                line_send[n, k] = jnp.concatenate(
                    [near[k * part :][:part], total[k * rest :][:rest]], axis=0
                ).astype(BF16)
            for m, peer in enumerate(x_peers):
                remote(
                    line_send.at[n, lax.rem(peer[0], pairs)],
                    line_recv.at[n, m],
                    peer,
                    line_out,
                    second[c],
                ).start()
    sent.append((pair_out, pair_recv))
    sent.append((line_out, line_recv))

    norm_out, norm_back = [next(sending) for _ in range(2)], [next(landing) for _ in range(2)]
    early = max(chunks - 2, 1) * chunk
    spans = [pl.ds(0, early), pl.ds(early, width + KMAX - early)]

    def share(n):
        mine = norm_all.at[i, :, spans[n]]
        for peer in row_peers:
            remote(mine, mine, peer, norm_out[n], norm_back[n]).start()

    for place, c in enumerate(order):
        span = slice(c * chunk, (c + 1) * chunk)
        if c < along_x:
            await_all(recv_sem, second[c], pair_recv.at[c])
            gradient = pair_send[c, z].astype(F32) + pair_recv[c].astype(F32)
        else:
            n = c - along_x
            await_all(recv_sem, second[c], line_recv.at[n])
            gradient = line_send[n, x].astype(F32) + jnp.sum(line_recv[n].astype(F32), axis=0)
        stepped = carry_all[:, span] + STEP_SIZE * gradient
        norm_all[i, :, place * chunk : (place + 1) * chunk] = jnp.sum(
            stepped * stepped, axis=0, keepdims=True
        )
        if place == chunks - 1:
            pl.when(follow)(lambda: await_all(recv_sem, total_back, energy_sum))
            norm_all[i, :, width:] = energy_sum[...]
            share(1)
        elif (place + 1) * chunk == early:
            share(0)
        settled = stepped * mask_all[:, span]
        for n, yy in enumerate(y_order):
            kept_out[rows_of(0, yy), span] = settled[n * part : (n + 1) * part]

    for n in range(2):
        others = norm_all.at[pl.ds(0, rows - 1), :, spans[n]]
        sent.append((norm_out[n], others))
        await_all(recv_sem, norm_back[n], others)
    summed = jnp.sum(norm_all[...], axis=0)
    for place, c in enumerate(order):
        sums_out[:, c * chunk : (c + 1) * chunk] = summed[:, place * chunk : (place + 1) * chunk]
    sums_out[:, width:] = summed[:, width:]

    pl.when(loop)(
        lambda: await_all(send_sem, first_out, first_send.at[pl.ds(0, far - 1)])
    )
    pl.when(no_loop)(lambda: await_all(send_sem, first_out, first_send))
    for out, ref in sent:
        await_all(send_sem, out, ref)

    @pl.when(lead)
    def _():
        for t in range(steps - 1):
            await_all(send_sem, kept_out_sem[t], kept.at[t, pl.ds(0, far - 1)])
        for k in range(rows):
            pl.when(jnp.logical_not(here[k]))(moves[k].wait_send)
        for out, ref in lead_sent:
            await_all(send_sem, out, ref())

    @pl.when(follow)
    def _():
        await_all(send_sem, kept_out_sem[steps - 2], kept.at[steps - 2, pl.ds(0, far)])


def finish(total_count, kept, sums, estimate, norms, energies):
    width = kept.shape[1]
    estimate[...] = kept[...]
    norms[...] = jnp.sqrt(sums[:, :width]).reshape(width)
    for t in range(energies.shape[0]):
        energies[t] = sums[0, width + t] / total_count


def solution(mesh, far=4, high=4, chunk=512, along_x=4):
    rows = mesh.shape["row"]

    def local(matrix, measured, support):
        depth, width = matrix.shape
        signals = measured.shape[0]
        group = signals // rows
        part = group // far
        party = rows * part
        rest = part * (far - 1)
        pairs = rows // 2
        steps = support.shape[0]
        turns = steps - 1
        span = min(chunk, width)
        chunks = width // span
        along_z = chunks - along_x
        in_vmem = pl.BlockSpec(memory_space=pltpu.VMEM)
        in_hbm = pl.BlockSpec(memory_space=pltpu.HBM)
        kept, sums = pl.pallas_call(
            functools.partial(kernel, (rows, far, high, along_x)),
            out_shape=(
                jax.ShapeDtypeStruct((group, width), F32),
                jax.ShapeDtypeStruct((1, width + KMAX), F32),
            ),
            in_specs=[in_hbm] * 3,
            out_specs=(in_vmem,) * 2,
            scratch_shapes=[
                pltpu.VMEM(support.shape, jnp.int32),
                pltpu.VMEM(measured.shape, F32),
                pltpu.VMEM((depth, width), BF16),
                pltpu.VMEM((steps, KMAX, 1), jnp.int32),
                pltpu.VMEM((turns, KMAX, 1), jnp.int32),
                pltpu.VMEM((turns, rows, KMAX, depth), BF16),
                pltpu.VMEM((turns - 1, depth, rows * KMAX), BF16),
                pltpu.VMEM((far, party, KMAX), BF16),
                pltpu.VMEM((rows, party, KMAX), BF16),
                pltpu.VMEM((turns, rows, party, KMAX), BF16),
                pltpu.VMEM((turns, rows - 1, party, KMAX), BF16),
                pltpu.VMEM((turns, rows, party, KMAX), BF16),
                pltpu.VMEM((party, KMAX), F32),
                pltpu.VMEM((turns, high, party, depth), BF16),
                pltpu.VMEM((rows, part, KMAX), F32),
                pltpu.VMEM((far, part, KMAX), F32),
                pltpu.VMEM((far, party, depth), BF16),
                pltpu.VMEM((far, 1, KMAX), F32),
                pltpu.VMEM((1, KMAX), F32),
                pltpu.VMEM((along_x, pairs, 2 * part, span), BF16),
                pltpu.VMEM((along_z, 2, pairs * part, span), BF16),
                pltpu.VMEM((along_x, pairs - 1, 2 * part, span), BF16),
                pltpu.VMEM((along_z, pairs * part, span), BF16),
                pltpu.VMEM((along_x, pairs, 2 * rest, span), BF16),
                pltpu.VMEM((along_z, 2, pairs * rest, span), BF16),
                pltpu.VMEM((along_x, pairs - 1, 2 * rest, span), BF16),
                pltpu.VMEM((along_z, pairs * rest, span), BF16),
                pltpu.VMEM((along_x, 2, group, span), BF16),
                pltpu.VMEM((along_x, group, span), BF16),
                pltpu.VMEM((along_z, pairs, group, span), BF16),
                pltpu.VMEM((along_z, pairs - 1, group, span), BF16),
                pltpu.VMEM((group, width), F32),
                pltpu.VMEM((1, width), F32),
                pltpu.VMEM((rows, 1, width + KMAX), F32),
                pltpu.SemaphoreType.DMA((chunks + 2,)),
                pltpu.SemaphoreType.DMA((25,)),
                pltpu.SemaphoreType.DMA((22 + 2 * chunks,)),
            ],
            compiler_params=pltpu.CompilerParams(
                collective_id=0, has_side_effects=True, vmem_limit_bytes=40 * 2**20
            ),
        )(*(pltpu.with_memory_space_constraint(a, pltpu.HBM) for a in (support, measured, matrix)))
        return pl.pallas_call(
            functools.partial(finish, float(signals * depth * rows)),
            out_shape=(
                jax.ShapeDtypeStruct((group, width), F32),
                jax.ShapeDtypeStruct((width,), F32),
                jax.ShapeDtypeStruct((steps,), F32),
            ),
            in_specs=[in_vmem] * 2,
            out_specs=(in_vmem, in_vmem, pl.BlockSpec(memory_space=pltpu.SMEM)),
            compiler_params=pltpu.CompilerParams(vmem_limit_bytes=4 * 2**20),
        )(kept, sums)

    return jax.shard_map(
        local,
        mesh=mesh,
        in_specs=(P("row", "col"), P(None, "row"), P()),
        out_specs=(P("row", "col"), P("col"), P()),
        check_vma=False,
    )
```
